128 devices in a mesh: ty: 2 (over core), tx: 64 (over z, y, x).
Axes of the slice: x: 4, y: 4, z: 4, core: 2. Of those that a mesh axis runs over, the one named last changes fastest.
Arguments:
- w_in: float32 [64, 2, 3, 128, 512], P('tx', 'ty')
- w_out: float32 [64, 2, 3, 512, 128], P('tx', 'ty')
- inputs: bfloat16 [64, 2, 7, 2048, 128], P('tx', 'ty')
- targets: bfloat16 [64, 2, 7, 2048, 128], P('tx', 'ty')
Outputs:
- output 1: float32 [64, 2, 3, 128, 512], P('tx', 'ty')
- output 2: float32 [64, 2, 3, 512, 128], P('tx', 'ty')
- output 3: float32 [64, 2, 3, 128, 512], P('tx', 'ty')
- output 4: float32 [64, 2, 3, 512, 128], P('tx', 'ty')
All inputs are finite; a program needn't handle non-finite values.
Results may differ from the reference program's by a relative error of at most 0.00525345.
Values are sent between devices in bfloat16 or wider.
A program may use at most 1 GiB of HBM per device.

```python
import jax
import jax.numpy as jnp
from jax import lax

TX = 64
TY = 2
LAYERS = 3
D = 128
FF = 512
ROWS = 2048
STEPS = 6
EPS = 1e-6
LEARN_RATE = 0.125


def setup_inputs(seed: int = 0) -> dict:
    root_key = jax.random.key(seed)
    key_list = jax.random.split(root_key, 6)
    base_in = jax.random.normal(key_list[0], (LAYERS, D, FF), jnp.float32)
    own_in = jax.random.normal(key_list[1], (TX, TY, LAYERS, D, FF), jnp.float32)
    w_in = (base_in[None, None] + 0.5 * own_in) * (D ** -0.5)
    base_out = jax.random.normal(key_list[2], (LAYERS, FF, D), jnp.float32)
    own_out = jax.random.normal(key_list[3], (TX, TY, LAYERS, FF, D), jnp.float32)
    w_out = (base_out[None, None] + 0.5 * own_out) * (FF ** -0.5)
    inputs = jax.random.normal(key_list[4], (TX, TY, STEPS + 1, ROWS, D), jnp.float32).astype(jnp.bfloat16)
    targets = jax.random.normal(key_list[5], (TX, TY, STEPS + 1, ROWS, D), jnp.float32).astype(jnp.bfloat16)
    return {'w_in': w_in, 'w_out': w_out, 'inputs': inputs, 'targets': targets}


def layer_step(hidden, weights):
    mat_in, mat_out = weights
    hidden_f32 = hidden.astype(jnp.float32)
    inv_rms = lax.rsqrt(jnp.mean(hidden_f32 * hidden_f32, axis=-1, keepdims=True) + EPS)
    normed = (hidden_f32 * inv_rms).astype(jnp.bfloat16)
    pre_act = jnp.dot(normed, mat_in.astype(jnp.bfloat16), preferred_element_type=jnp.float32)
    gelu_out = jax.nn.gelu(pre_act).astype(jnp.bfloat16)
    mlp_out = jnp.dot(gelu_out, mat_out.astype(jnp.bfloat16), preferred_element_type=jnp.float32)
    return (hidden_f32 + mlp_out).astype(jnp.bfloat16), None


def local_loss(w_in, w_out, batch_in, batch_tgt):
    last_hidden, _ = lax.scan(layer_step, batch_in, (w_in, w_out))
    resid_err = last_hidden.astype(jnp.float32) - batch_tgt.astype(jnp.float32)
    return jnp.mean(resid_err * resid_err)


local_grads = jax.grad(local_loss, argnums=(0, 1))


def gossip_mix(values):
    sent_copy = values.astype(jnp.bfloat16).astype(jnp.float32)
    summed = values + jnp.roll(sent_copy, 1, axis=0)
    summed = summed + jnp.roll(sent_copy, -1, axis=0)
    summed = summed + jnp.roll(sent_copy, 1, axis=1)
    summed = summed + jnp.roll(sent_copy, -1, axis=1)
    return summed / 5.0


def reference(w_in, w_out, inputs, targets):
    cell_count = TX * TY
    step_size = LEARN_RATE

    def one_cell(operands):
        return local_grads(operands[0], operands[1], operands[2], operands[3])

    def all_grads(p_in, p_out, step_idx):
        batch_in = lax.dynamic_index_in_dim(inputs, step_idx, axis=2, keepdims=False).reshape((cell_count, ROWS, D))
        batch_tgt = lax.dynamic_index_in_dim(targets, step_idx, axis=2, keepdims=False).reshape((cell_count, ROWS, D))
        grad_in, grad_out = lax.map(one_cell, (p_in.reshape((cell_count, LAYERS, D, FF)), p_out.reshape((cell_count, LAYERS, FF, D)), batch_in, batch_tgt))
        return grad_in.reshape(p_in.shape), grad_out.reshape(p_out.shape)

    first_in, first_out = all_grads(w_in, w_out, 0)

    def step_body(carried, step_idx):
        p_in, p_out, y_in, y_out, old_in, old_out = carried
        p_in = gossip_mix(p_in) - step_size * y_in
        p_out = gossip_mix(p_out) - step_size * y_out
        new_gin, new_gout = all_grads(p_in, p_out, step_idx)
        y_in = gossip_mix(y_in) + new_gin - old_in
        y_out = gossip_mix(y_out) + new_gout - old_out
        return (p_in, p_out, y_in, y_out, new_gin, new_gout), None

    final_state, _ = lax.scan(step_body, (w_in, w_out, first_in, first_out, first_in, first_out), jnp.arange(1, STEPS + 1))
    return (final_state[0], final_state[1], final_state[2], final_state[3])
```

```python
import functools

import jax
import jax.numpy as jnp
from jax import lax
from jax.experimental import pallas as pl
from jax.experimental.pallas import tpu as pltpu
from jax.sharding import PartitionSpec as P

EPS = 1e-6
LEARN_RATE = 0.125
F32 = jnp.float32
BF16 = jnp.bfloat16
C0 = 0.7978845608028654
C1 = 0.7978845608028654 * 0.044715
TILE = 256


def dot(a, b, dims):
    return lax.dot_general(a, b, (dims, ((), ())), preferred_element_type=F32)


def forward_tile(rows, h_in, win, wout, u_ref, inv_ref, gp_ref, a_ref):
    d = h_in.shape[-1]
    hf = h_in[rows, :].astype(F32)
    ms = jnp.sum(hf * hf, axis=-1, keepdims=True) * (1.0 / d)
    inv = jnp.broadcast_to(lax.rsqrt(ms + EPS), hf.shape)
    inv_ref[rows, :] = inv
    u = (hf * inv).astype(BF16)
    u_ref[rows, :] = u
    z = dot(u, win[...], ((1,), (0,)))
    z2 = z * z
    t = jnp.tanh(z * (C0 + C1 * z2))
    w = 0.5 + 0.5 * t
    a = (z * w).astype(BF16)
    a_ref[rows, :] = a
    gp_ref[rows, :] = w + (w - w * w) * (z * (2.0 * C0 + (6.0 * C1) * z2))
    mlp = dot(a, wout[...], ((1,), (0,)))
    return (hf + mlp).astype(BF16)


def backward_tile(rows, first, h_in, win, wout, u_ref, inv_ref, gp_ref, a_ref, dh_ref, dwin, dwoutt):
    d = dh_ref[rows, :]
    da = dot(d, wout[...], ((1,), (1,))).astype(BF16).astype(F32)
    dz = (da * gp_ref[rows, :]).astype(BF16)
    dwoutt[...] += dot(d, a_ref[rows, :], ((0,), (0,)))
    dwin[...] += dot(u_ref[rows, :], dz, ((0,), (0,)))
    if not first:
        du = dot(dz, win[...], ((1,), (1,))).astype(BF16).astype(F32)
        hf = h_in[rows, :].astype(F32)
        inv = inv_ref[rows, :]
        s = jnp.sum(du * hf, axis=-1, keepdims=True) * (-1.0 / hf.shape[-1])
        dhf = d.astype(F32) + du * inv + hf * (inv * inv * inv * s)
        dh_ref[rows, :] = dhf.astype(BF16)


def kernel(dims, w_in, w_out, x_hbm, t_hbm, o_pin, o_pout, o_yin, o_yout,
           p_in, p_out, y_in, y_out, pb_in, pb_out, yb_in, yb_out, r_in, r_out, g_in, g_out,
           dw_in, dw_outt, xb, tb, hid, u_all, inv_all, gp_all, a_all, dh,
           lsem, xsem, ssem, rsem):
    size_x, size_y, layers, steps = dims
    rows_n = xb.shape[1]
    me_x = lax.axis_index('tx')
    me_y = lax.axis_index('ty')
    right = lax.rem(me_x + 1, size_x)
    left = lax.rem(me_x + size_x - 1, size_x)
    other = lax.rem(me_y + 1, size_y)
    peers = ({'tx': right, 'ty': me_y}, {'tx': left, 'ty': me_y}, {'tx': me_x, 'ty': other})
    chunks = [(l, k) for l in range(layers) for k in range(2)]
    pst, yst, pbs, ybs, rcv, gold = (p_in, p_out), (y_in, y_out), (pb_in, pb_out), (yb_in, yb_out), (r_in, r_out), (g_in, g_out)

    def loads():
        return [pltpu.make_async_copy(w_in, p_in, lsem.at[0]), pltpu.make_async_copy(w_out, p_out, lsem.at[1])]

    def batch(t, slot):
        return [pltpu.make_async_copy(x_hbm.at[t], xb.at[slot], xsem.at[slot, 0]),
                pltpu.make_async_copy(t_hbm.at[t], tb.at[slot], xsem.at[slot, 1])]

    def send(kind, par, c, d):
        l, k = chunks[c]
        src = (pbs, ybs)[kind][k].at[l]
        return pltpu.make_async_remote_copy(
            src_ref=src, dst_ref=rcv[k].at[kind, par, d, l], send_sem=ssem.at[kind, d, c],
            recv_sem=rsem.at[kind, par, d, c], device_id=peers[d], device_id_type=pl.DeviceIdType.MESH)

    def start_sends(kind, par, c):
        for d in range(3):
            send(kind, par, c, d).start()

    def wait_chunk(kind, par, c):
        for d in range(3):
            send(kind, par, c, d).wait()

    def mix(v, kind, par, l, k, sl):
        s = v + rcv[k][kind, par, 0, l, sl, :].astype(F32)
        s = s + rcv[k][kind, par, 1, l, sl, :].astype(F32)
        n = rcv[k][kind, par, 2, l, sl, :].astype(F32)
        return (s + n + n) * 0.2

    for cp in loads() + batch(0, 0):
        cp.start()
    barrier = pltpu.get_barrier_semaphore()
    for peer in peers:
        pl.semaphore_signal(barrier, inc=1, device_id=peer, device_id_type=pl.DeviceIdType.MESH)
    for cp in loads():
        cp.wait()
    for l, k in chunks:
        pbs[k][l] = pst[k][l].astype(BF16)
    pl.semaphore_wait(barrier, 3)
    for c in range(len(chunks)):
        start_sends(0, 0, c)

    def step(t, carry):
        slot = lax.rem(t, 2)
        nxt = 1 - slot
        for cp in batch(t, slot):
            cp.wait()

        @pl.when(t < steps)
        def _():
            for cp in batch(t + 1, nxt):
                cp.start()

        tiles = rows_n // TILE
        for l in range(layers):
            h_in = xb.at[slot] if l == 0 else hid.at[l - 1]

            def fwd(i, c, l=l, h_in=h_in):
                rows = pl.ds(pl.multiple_of(i * TILE, TILE), TILE)
                h = forward_tile(rows, h_in, pb_in.at[l], pb_out.at[l], u_all.at[l], inv_all.at[l], gp_all.at[l], a_all.at[l])
                if l + 1 < layers:
                    hid[l, rows, :] = h
                else:
                    err = h.astype(F32) - tb[slot, rows, :].astype(F32)
                    dh[rows, :] = (err * (2.0 / (rows_n * h.shape[-1]))).astype(BF16)
                return c

            lax.fori_loop(0, tiles, fwd, 0)
        for l in reversed(range(layers)):
            h_in = xb.at[slot] if l == 0 else hid.at[l - 1]
            dw_in[l] = jnp.zeros_like(dw_in[l])
            dw_outt[l] = jnp.zeros_like(dw_outt[l])

            def bwd(i, c, l=l, h_in=h_in):
                rows = pl.ds(pl.multiple_of(i * TILE, TILE), TILE)
                backward_tile(rows, l == 0, h_in, pb_in.at[l], pb_out.at[l], u_all.at[l], inv_all.at[l], gp_all.at[l],
                              a_all.at[l], dh, dw_in.at[l], dw_outt.at[l])
                return c

            lax.fori_loop(0, tiles, bwd, 0)

        def new_grad(l, k):
            g = dw_in[l] if k == 0 else dw_outt[l].T
            return g.astype(BF16).astype(F32)

        for c, (l, k) in enumerate(chunks):
            g = new_grad(l, k)

            @pl.when(t == 0)
            def _():
                yst[k][l] = g

            @pl.when(t > 0)
            def _():
                wait_chunk(1, nxt, c)
                yst[k][l] = (mix(yst[k][l], 1, nxt, l, k, slice(None)) + g) - gold[k][l].astype(F32)

            gold[k][l] = g.astype(BF16)

            @pl.when(t < steps)
            def _():
                ybs[k][l] = yst[k][l].astype(BF16)
                if c > 0:
                    start_sends(1, slot, c - 1)

        @pl.when(t < steps)
        def _():
            for c, (l, k) in enumerate(chunks):
                wait_chunk(0, slot, c)
                pn = mix(pst[k][l], 0, slot, l, k, slice(None)) - LEARN_RATE * yst[k][l]
                pst[k][l] = pn
                pbs[k][l] = pn.astype(BF16)
                if c == 0:
                    start_sends(1, slot, len(chunks) - 1)
                else:
                    @pl.when(t < steps - 1)
                    def _():
                        start_sends(0, nxt, c - 1)

            @pl.when(t < steps - 1)
            def _():
                start_sends(0, nxt, len(chunks) - 1)

            @pl.when(t == steps - 1)
            def _():
                for cp in outs_p():
                    cp.start()
        return carry

    def outs_p():
        return [pltpu.make_async_copy(p_in, o_pin, lsem.at[0]), pltpu.make_async_copy(p_out, o_pout, lsem.at[1])]

    lax.fori_loop(0, steps + 1, step, 0)
    outs_y = [pltpu.make_async_copy(y_in, o_yin, lsem.at[2]), pltpu.make_async_copy(y_out, o_yout, lsem.at[3])]
    for cp in outs_y:
        cp.start()
    for cp in outs_p() + outs_y:
        cp.wait()


def solution(mesh):
    size_x = mesh.shape['tx']
    size_y = mesh.shape['ty']

    def device_fn(w_in, w_out, inputs, targets):
        _, _, layers, d, ff = w_in.shape
        steps = inputs.shape[2] - 1
        rows = inputs.shape[3]
        si, so = (layers, d, ff), (layers, ff, d)
        vm = pltpu.VMEM
        sem = pltpu.SemaphoreType.DMA
        any_spec = pl.BlockSpec(memory_space=pl.ANY)
        outs = pl.pallas_call(
            functools.partial(kernel, (size_x, size_y, layers, steps)),
            out_shape=[jax.ShapeDtypeStruct(si, F32), jax.ShapeDtypeStruct(so, F32)] * 2,
            in_specs=[any_spec] * 4,
            out_specs=[any_spec] * 4,
            scratch_shapes=[
                vm(si, F32), vm(so, F32), vm(si, F32), vm(so, F32),
                vm(si, BF16), vm(so, BF16), vm(si, BF16), vm(so, BF16),
                vm((2, 2, 3) + si, BF16), vm((2, 2, 3) + so, BF16), vm(si, BF16), vm(so, BF16),
                vm(si, F32), vm(si, F32),
                vm((2, rows, d), BF16), vm((2, rows, d), BF16), vm((layers - 1, rows, d), BF16),
                vm((layers, rows, d), BF16), vm((layers, rows, d), F32), vm((layers, rows, ff), F32),
                vm((layers, rows, ff), BF16), vm((rows, d), BF16),
                sem((4,)), sem((2, 2)), sem((2, 3, 2 * layers)), sem((2, 2, 3, 2 * layers)),
            ],
            compiler_params=pltpu.CompilerParams(collective_id=0, has_side_effects=True, vmem_limit_bytes=64000000),
        )(w_in[0, 0], w_out[0, 0], inputs[0, 0], targets[0, 0])
        return tuple(o[None, None] for o in outs)

    block_spec = P('tx', 'ty')
    return jax.shard_map(device_fn, mesh=mesh, in_specs=(block_spec,) * 4, out_specs=(block_spec,) * 4, check_vma=False)
```

```python
import functools

import jax
import jax.numpy as jnp
from jax import lax
from jax.experimental import pallas as pl
from jax.experimental.pallas import tpu as pltpu
from jax.sharding import PartitionSpec as P

EPS = 1e-6
LEARN_RATE = 0.125
F32 = jnp.float32
BF16 = jnp.bfloat16
C0 = 0.7978845608028654
C1 = 0.7978845608028654 * 0.044715
TILE = 1024


def dot(a, b, dims):
    return lax.dot_general(a, b, (dims, ((), ())), preferred_element_type=F32)


def forward_tile(rows, h_in, win, wout, u_ref, inv_ref, gp_ref, a_ref):
    d = h_in.shape[-1]
    hf = h_in[rows, :].astype(F32)
    ms = jnp.sum(hf * hf, axis=-1, keepdims=True) * (1.0 / d)
    inv = jnp.broadcast_to(lax.rsqrt(ms + EPS), hf.shape)
    inv_ref[rows, :] = inv
    u = (hf * inv).astype(BF16)
    u_ref[rows, :] = u
    z = dot(u, win[...], ((1,), (0,)))
    z2 = z * z
    t = jnp.tanh(z * (C0 + C1 * z2))
    w = 0.5 + 0.5 * t
    a = (z * w).astype(BF16)
    a_ref[rows, :] = a
    gp_ref[rows, :] = w + (w - w * w) * (z * (2.0 * C0 + (6.0 * C1) * z2))
    mlp = dot(a, wout[...], ((1,), (0,)))
    return (hf + mlp).astype(BF16)


def backward_tile(rows, first, h_in, win, wout, u_ref, inv_ref, gp_ref, a_ref, dh_ref, dwin, dwoutt):
    d = dh_ref[rows, :]
    da = dot(d, wout[...], ((1,), (1,))).astype(BF16).astype(F32)
    dz = (da * gp_ref[rows, :]).astype(BF16)
    dwoutt[...] += dot(d, a_ref[rows, :], ((0,), (0,)))
    dwin[...] += dot(u_ref[rows, :], dz, ((0,), (0,)))
    if not first:
        du = dot(dz, win[...], ((1,), (1,))).astype(BF16).astype(F32)
        hf = h_in[rows, :].astype(F32)
        inv = inv_ref[rows, :]
        s = jnp.sum(du * hf, axis=-1, keepdims=True) * (-1.0 / hf.shape[-1])
        dhf = d.astype(F32) + du * inv + hf * (inv * inv * inv * s)
        dh_ref[rows, :] = dhf.astype(BF16)


def kernel(dims, w_in, w_out, x_hbm, t_hbm, p_in, p_out, y_in, y_out, pb_in, pb_out, yb_in, yb_out, r_in, r_out, g_in, g_out,
           dw_in, dw_outt, xb, tb, hid, u_all, inv_all, gp_all, a_all, dh,
           lsem, xsem, ssem, rsem):
    size_x, size_y, layers, steps = dims
    rows_n = xb.shape[1]
    me_x = lax.axis_index('tx')
    me_y = lax.axis_index('ty')
    right = lax.rem(me_x + 1, size_x)
    left = lax.rem(me_x + size_x - 1, size_x)
    other = lax.rem(me_y + 1, size_y)
    peers = ({'tx': right, 'ty': me_y}, {'tx': left, 'ty': me_y}, {'tx': me_x, 'ty': other})
    chunks = [(l, k) for l in range(layers) for k in range(2)]
    pst, yst, pbs, ybs, rcv, gold = (p_in, p_out), (y_in, y_out), (pb_in, pb_out), (yb_in, yb_out), (r_in, r_out), (g_in, g_out)

    def loads():
        return [pltpu.make_async_copy(w_in, p_in, lsem.at[0]), pltpu.make_async_copy(w_out, p_out, lsem.at[1])]

    def batch(t, slot):
        return [pltpu.make_async_copy(x_hbm.at[t], xb.at[slot], xsem.at[slot, 0]),
                pltpu.make_async_copy(t_hbm.at[t], tb.at[slot], xsem.at[slot, 1])]

    def send(kind, par, c, d):
        l, k = chunks[c]
        src = (pbs, ybs)[kind][k].at[l]
        return pltpu.make_async_remote_copy(
            src_ref=src, dst_ref=rcv[k].at[kind, par, d, l], send_sem=ssem.at[kind, d, c],
            recv_sem=rsem.at[kind, par, d, c], device_id=peers[d], device_id_type=pl.DeviceIdType.MESH)

    def start_sends(kind, par, c):
        for d in range(3):
            send(kind, par, c, d).start()

    def wait_chunk(kind, par, c):
        for d in range(3):
            send(kind, par, c, d).wait()

    def mix(v, kind, par, l, k, sl):
        s = v + rcv[k][kind, par, 0, l, sl, :].astype(F32)
        s = s + rcv[k][kind, par, 1, l, sl, :].astype(F32)
        n = rcv[k][kind, par, 2, l, sl, :].astype(F32)
        return (s + n + n) * 0.2

    for cp in loads() + batch(0, 0):
        cp.start()
    barrier = pltpu.get_barrier_semaphore()
    for peer in peers:
        pl.semaphore_signal(barrier, inc=1, device_id=peer, device_id_type=pl.DeviceIdType.MESH)
    for cp in loads():
        cp.wait()
    for l, k in chunks:
        pbs[k][l] = pst[k][l].astype(BF16)
    pl.semaphore_wait(barrier, 3)
    for c in range(len(chunks)):
        start_sends(0, 0, c)

    def step(t, carry):
        slot = lax.rem(t, 2)
        nxt = 1 - slot
        for cp in batch(t, slot):
            cp.wait()

        @pl.when(t < steps)
        def _():
            for cp in batch(t + 1, nxt):
                cp.start()

        tiles = rows_n // TILE
        for l in range(layers):
            h_in = xb.at[slot] if l == 0 else hid.at[l - 1]

            def fwd(i, c, l=l, h_in=h_in):
                rows = pl.ds(pl.multiple_of(i * TILE, TILE), TILE)
                h = forward_tile(rows, h_in, pb_in.at[l], pb_out.at[l], u_all.at[l], inv_all.at[l], gp_all.at[l], a_all.at[l])
                if l + 1 < layers:
                    hid[l, rows, :] = h
                else:
                    err = h.astype(F32) - tb[slot, rows, :].astype(F32)
                    dh[rows, :] = (err * (2.0 / (rows_n * h.shape[-1]))).astype(BF16)
                return c

            lax.fori_loop(0, tiles, fwd, 0)
        for l in reversed(range(layers)):
            h_in = xb.at[slot] if l == 0 else hid.at[l - 1]
            dw_in[l] = jnp.zeros_like(dw_in[l])
            dw_outt[l] = jnp.zeros_like(dw_outt[l])

            def bwd(i, c, l=l, h_in=h_in):
                rows = pl.ds(pl.multiple_of(i * TILE, TILE), TILE)
                backward_tile(rows, l == 0, h_in, pb_in.at[l], pb_out.at[l], u_all.at[l], inv_all.at[l], gp_all.at[l],
                              a_all.at[l], dh, dw_in.at[l], dw_outt.at[l])
                return c

            lax.fori_loop(0, tiles, bwd, 0)

        def new_grad(l, k):
            g = dw_in[l] if k == 0 else dw_outt[l].T
            return g.astype(BF16).astype(F32)

        for c, (l, k) in enumerate(chunks):
            g = new_grad(l, k)

            @pl.when(t == 0)
            def _():
                yst[k][l] = g

            @pl.when(t > 0)
            def _():
                wait_chunk(1, nxt, c)
                yst[k][l] = (mix(yst[k][l], 1, nxt, l, k, slice(None)) + g) - gold[k][l].astype(F32)

            gold[k][l] = g.astype(BF16)

            @pl.when(t < steps)
            def _():
                ybs[k][l] = yst[k][l].astype(BF16)
                if c > 0:
                    start_sends(1, slot, c - 1)

        @pl.when(t < steps)
        def _():
            for c, (l, k) in enumerate(chunks):
                wait_chunk(0, slot, c)
                pn = mix(pst[k][l], 0, slot, l, k, slice(None)) - LEARN_RATE * yst[k][l]
                pst[k][l] = pn
                pbs[k][l] = pn.astype(BF16)
                if c == 0:
                    start_sends(1, slot, len(chunks) - 1)
                else:
                    @pl.when(t < steps - 1)
                    def _():
                        start_sends(0, nxt, c - 1)

            @pl.when(t < steps - 1)
            def _():
                start_sends(0, nxt, len(chunks) - 1)
        return carry

    lax.fori_loop(0, steps + 1, step, 0)


def flush(*refs):
    copies = [pltpu.make_async_copy(refs[n], refs[4 + n], refs[8].at[n]) for n in range(4)]
    for cp in copies:
        cp.start()
    for cp in copies:
        cp.wait()


def solution(mesh):
    size_x = mesh.shape['tx']
    size_y = mesh.shape['ty']

    def device_fn(w_in, w_out, inputs, targets):
        _, _, layers, d, ff = w_in.shape
        steps = inputs.shape[2] - 1
        rows = inputs.shape[3]
        si, so = (layers, d, ff), (layers, ff, d)
        vm = pltpu.VMEM
        sem = pltpu.SemaphoreType.DMA
        any_spec = pl.BlockSpec(memory_space=pl.ANY)
        outs = pl.pallas_call(
            functools.partial(kernel, (size_x, size_y, layers, steps)),
            out_shape=[vm(si, F32), vm(so, F32)] * 2,
            in_specs=[any_spec] * 4,
            out_specs=[pl.BlockSpec(memory_space=pltpu.VMEM)] * 4,
            scratch_shapes=[
                vm(si, BF16), vm(so, BF16), vm(si, BF16), vm(so, BF16),
                vm((2, 2, 3) + si, BF16), vm((2, 2, 3) + so, BF16), vm(si, BF16), vm(so, BF16),
                vm(si, F32), vm(si, F32),
                vm((2, rows, d), BF16), vm((2, rows, d), BF16), vm((layers - 1, rows, d), BF16),
                vm((layers, rows, d), BF16), vm((layers, rows, d), F32), vm((layers, rows, ff), F32),
                vm((layers, rows, ff), BF16), vm((rows, d), BF16),
                sem((2,)), sem((2, 2)), sem((2, 3, 2 * layers)), sem((2, 2, 3, 2 * layers)),
            ],
            compiler_params=pltpu.CompilerParams(collective_id=0, has_side_effects=True, vmem_limit_bytes=56000000),
        )(w_in[0, 0], w_out[0, 0], inputs[0, 0], targets[0, 0])
        outs = pl.pallas_call(
            flush,
            out_shape=[jax.ShapeDtypeStruct(o.shape, o.dtype) for o in outs],
            in_specs=[pl.BlockSpec(memory_space=pltpu.VMEM)] * 4,
            out_specs=[any_spec] * 4,
            scratch_shapes=[sem((4,))],
        )(*[pltpu.with_memory_space_constraint(o, pltpu.VMEM) for o in outs])
        return tuple(o[None, None] for o in outs)

    block_spec = P('tx', 'ty')
    return jax.shard_map(device_fn, mesh=mesh, in_specs=(block_spec,) * 4, out_specs=(block_spec,) * 4, check_vma=False)
```

```python
import functools

import jax
import jax.numpy as jnp
from jax import lax
from jax.experimental import pallas as pl
from jax.experimental.pallas import tpu as pltpu
from jax.sharding import PartitionSpec as P

EPS = 1e-6
LEARN_RATE = 0.125
F32 = jnp.float32
BF16 = jnp.bfloat16
C0 = 0.7978845608028654
C1 = 0.7978845608028654 * 0.044715
TILE = 1024
LINE = 4
MESH = pl.DeviceIdType.MESH


def dot(a, b, dims):
    return lax.dot_general(a, b, (dims, ((), ())), preferred_element_type=F32)


def forward_tile(rows, h_in, win, wout, u_ref, inv_ref, gp_ref, a_ref):
    d = h_in.shape[-1]
    hf = h_in[rows, :].astype(F32)
    ms = jnp.sum(hf * hf, axis=-1, keepdims=True) * (1.0 / d)
    inv = jnp.broadcast_to(lax.rsqrt(ms + EPS), hf.shape)
    inv_ref[rows, :] = inv
    u = (hf * inv).astype(BF16)
    u_ref[rows, :] = u
    z = dot(u, win[...], ((1,), (0,)))
    z2 = z * z
    t = jnp.tanh(z * (C0 + C1 * z2))
    w = 0.5 + 0.5 * t
    a = (z * w).astype(BF16)
    a_ref[rows, :] = a
    gp_ref[rows, :] = w + (w - w * w) * (z * (2.0 * C0 + (6.0 * C1) * z2))
    mlp = dot(a, wout[...], ((1,), (0,)))
    return (hf + mlp).astype(BF16)


def backward_tile(rows, first, h_in, win, wout, u_ref, inv_ref, gp_ref, a_ref, dh_ref, dwin, dwoutt):
    d = dh_ref[rows, :]
    da = dot(d, wout[...], ((1,), (1,))).astype(BF16).astype(F32)
    dz = (da * gp_ref[rows, :]).astype(BF16)
    dwoutt[...] += dot(d, a_ref[rows, :], ((0,), (0,)))
    dwin[...] += dot(u_ref[rows, :], dz, ((0,), (0,)))
    if not first:
        du = dot(dz, win[...], ((1,), (1,))).astype(BF16).astype(F32)
        hf = h_in[rows, :].astype(F32)
        inv = inv_ref[rows, :]
        s = jnp.sum(du * hf, axis=-1, keepdims=True) * (-1.0 / hf.shape[-1])
        dhf = d.astype(F32) + du * inv + hf * (inv * inv * inv * s)
        dh_ref[rows, :] = dhf.astype(BF16)


def kernel(dims, w_in, w_out, x_hbm, t_hbm, p_in, p_out, y_in, y_out,
           pb_in, pb_out, yb_in, yb_out, r_in, r_out, g_in, g_out,
           ps_in, ps_out, ys_in, ys_out, sp_in, sp_out, sy_in, sy_out,
           gb_in, gb_out, gs_in, gs_out, re_in, re_out, rp_in, rp_out,
           dw_in, dw_outt, xb, tb, hid, u_all, inv_all, gp_all, a_all, dh,
           lsem, xsem, ssem, rsem, esend, erecv, gsend, grecv, psend, precv, fsend, frecv):
    size_x, size_y, layers, steps = dims
    rows_n = xb.shape[1]
    me_x = lax.axis_index('tx')
    me_y = lax.axis_index('ty')
    pos = lax.rem(me_x, LINE)
    line = me_x - pos

    def along(off):
        return {'tx': lax.rem(me_x + size_x + off, size_x), 'ty': me_y}

    other = {'tx': me_x, 'ty': lax.rem(me_y + 1, size_y)}
    near = (along(1), along(-1), other)
    ends = (along(LINE), along(-LINE), other)
    mates = [{'tx': line + lax.rem(pos + k, LINE), 'ty': me_y} for k in range(1, LINE)]
    p_st, y_st, pb, yb, rcv, gold = (p_in, p_out), (y_in, y_out), (pb_in, pb_out), (yb_in, yb_out), (r_in, r_out), (g_in, g_out)
    ps, ys, sp, sy = (ps_in, ps_out), (ys_in, ys_out), (sp_in, sp_out), (sy_in, sy_out)
    gb, gs, redge, rpart = (gb_in, gb_out), (gs_in, gs_out), (re_in, re_out), (rp_in, rp_out)
    blk = tuple(ref.shape[1] // LINE for ref in ps)

    def block(k, b):
        return pl.ds(pl.multiple_of(b * blk[k], blk[k]), blk[k])

    def remote(src, dst, s, r, dev):
        return pltpu.make_async_remote_copy(src_ref=src, dst_ref=dst, send_sem=s, recv_sem=r, device_id=dev, device_id_type=MESH)

    def start(copies):
        for cp in copies:
            cp.start()

    def wait(copies):
        for cp in copies:
            cp.wait()

    def loads():
        return [pltpu.make_async_copy(w_in, p_in, lsem.at[0]), pltpu.make_async_copy(w_out, p_out, lsem.at[1])]

    def batch(t, slot):
        return [pltpu.make_async_copy(x_hbm.at[t], xb.at[slot], xsem.at[slot, 0]),
                pltpu.make_async_copy(t_hbm.at[t], tb.at[slot], xsem.at[slot, 1])]

    def bulk(kind, par):
        return [remote((pb[k].at[0], yb[k])[kind], rcv[k].at[kind, par, d], ssem.at[kind, d, k], rsem.at[kind, par, d, k], near[d])
                for k in range(2) for d in range(3)]

    def mix0(v, kind, par, k):
        s = v + rcv[k][kind, par, 0].astype(F32)
        s = s + rcv[k][kind, par, 1].astype(F32)
        n = rcv[k][kind, par, 2].astype(F32)
        return (s + n + n) * 0.2

    def edges(kind, par, lb):
        out = []
        for k in range(2):
            src = (sp, sy)[kind][k].at[par, lb]
            m = lb * 2 + k
            for d in range(3):
                part = (src.at[pl.ds((LINE - 1) * blk[k], blk[k])], src.at[pl.ds(0, blk[k])], src)[d]
                dst = redge[k].at[kind, par, d, lb] if d < 2 else rpart[k].at[kind, par, lb]
                out.append(remote(part, dst, esend.at[kind, d, m], erecv.at[kind, par, d, m], ends[d]))
        return out

    def swap(src, dst, send, recv, lb):
        out = []
        for k in range(2):
            for n, dev in enumerate(mates):
                out.append(remote(src[k].at[block(k, lax.rem(pos + n + 1, LINE))], dst[k].at[block(k, pos)],
                                  send.at[lb * 2 + k, n], recv.at[lb * 2 + k, n], dev))
        return out

    def g_swap(par, lb):
        return swap([g.at[par, lb] for g in gb], [g.at[par, lb] for g in gs], gsend, grecv, lb)

    def p_swap(par, lb):
        return swap([s.at[par, lb] for s in sp], [w.at[lb + 1] for w in pb], psend, precv, lb)

    def p_swap_f32(lb):
        return swap([s.at[lb] for s in ps], [w.at[lb + 1] for w in p_st], psend, precv, lb)

    def y_swap_f32(lb):
        return swap([s.at[lb] for s in ys], [w.at[lb + 1] for w in y_st], fsend, frecv, lb)

    def first_swap(lb):
        return swap([w.at[lb + 1] for w in p_st], [s.at[lb] for s in ps], fsend, frecv, lb)

    def mix_b(v, kind, par, lb, k, b):
        src = (sp, sy)[kind][k]
        rows = slice(b * blk[k], (b + 1) * blk[k])
        lo = redge[k][kind, par, 0, lb] if b == 0 else src[par, lb, (b - 1) * blk[k]:b * blk[k], :]
        hi = redge[k][kind, par, 1, lb] if b == LINE - 1 else src[par, lb, (b + 1) * blk[k]:(b + 2) * blk[k], :]
        n = rpart[k][kind, par, lb, rows, :].astype(F32)
        return (v + lo.astype(F32) + hi.astype(F32) + n + n) * 0.2

    def own_rows(lb, t, slot, nxt):
        wait(g_swap(nxt, lb))
        wait(edges(0, nxt, lb))

        @pl.when(t >= 2)
        def _():
            wait(edges(1, slot, lb))

        for k in range(2):
            for b in range(LINE):
                rows = slice(b * blk[k], (b + 1) * blk[k])
                g = gs[k][nxt, lb, rows, :].astype(F32)

                @pl.when(t == 1)
                def _():
                    ys[k][lb, rows, :] = g

                @pl.when(t >= 2)
                def _():
                    ys[k][lb, rows, :] = (mix_b(ys[k][lb, rows, :], 1, slot, lb, k, b) + g) - gs[k][slot, lb, rows, :].astype(F32)

                y = ys[k][lb, rows, :]
                p = mix_b(ps[k][lb, rows, :], 0, nxt, lb, k, b) - LEARN_RATE * y
                ps[k][lb, rows, :] = p
                sp[k][slot, lb, rows, :] = p.astype(BF16)
                sy[k][nxt, lb, rows, :] = y.astype(BF16)

        @pl.when(t < steps)
        def _():
            for k in range(2):
                pb[k][lb + 1, block(k, pos), :] = sp[k][slot, lb, block(k, pos), :]
            start(p_swap(slot, lb))
            start(edges(0, slot, lb))

        @pl.when(t == steps)
        def _():
            for k in range(2):
                p_st[k][lb + 1, block(k, pos), :] = ps[k][lb, block(k, pos), :]
            start(p_swap_f32(lb))

        start(edges(1, nxt, lb))

    def last_trackers(lb, par):
        wait(edges(1, par, lb))
        for k in range(2):
            for b in range(LINE):
                rows = slice(b * blk[k], (b + 1) * blk[k])
                ys[k][lb, rows, :] = mix_b(ys[k][lb, rows, :], 1, par, lb, k, b)
            y_st[k][lb + 1, block(k, pos), :] = ys[k][lb, block(k, pos), :]
        start(y_swap_f32(lb))

    def take_weights(lb, t, slot):
        @pl.when(jnp.logical_and(t >= 1, t < steps))
        def _():
            wait(p_swap(slot, lb))

        @pl.when(t == steps)
        def _():
            wait(p_swap_f32(lb))
            for k in range(2):
                pb[k][lb + 1] = p_st[k][lb + 1].astype(BF16)

    start(loads() + batch(0, 0))
    barrier = pltpu.get_barrier_semaphore()
    for peer in mates + list(near) + list(ends[:2]):
        pl.semaphore_signal(barrier, inc=1, device_id=peer, device_id_type=MESH)
    wait(loads())
    pl.semaphore_wait(barrier, LINE + 4)
    for lb in range(layers - 1):
        start(first_swap(lb))
    for k in range(2):
        for l in range(layers):
            pb[k][l] = p_st[k][l].astype(BF16)
        for lb in range(layers - 1):
            ps[k][lb, block(k, pos), :] = p_st[k][lb + 1, block(k, pos), :]
    start(bulk(0, 0))

    def step(t, carry):
        slot = lax.rem(t, 2)
        nxt = 1 - slot
        tiles = rows_n // TILE
        wait(batch(t, slot))

        @pl.when(t < steps)
        def _():
            start(batch(t + 1, nxt))

        def fwd(i, l, h_in):
            rows = pl.ds(pl.multiple_of(i * TILE, TILE), TILE)
            h = forward_tile(rows, h_in, pb_in.at[l], pb_out.at[l], u_all.at[l], inv_all.at[l], gp_all.at[l], a_all.at[l])
            if l + 1 < layers:
                hid[l, rows, :] = h
            else:
                err = h.astype(F32) - tb[slot, rows, :].astype(F32)
                dh[rows, :] = (err * (2.0 / (rows_n * h.shape[-1]))).astype(BF16)

        def bwd(i, l, h_in):
            rows = pl.ds(pl.multiple_of(i * TILE, TILE), TILE)
            backward_tile(rows, l == 0, h_in, pb_in.at[l], pb_out.at[l], u_all.at[l], inv_all.at[l], gp_all.at[l],
                          a_all.at[l], dh, dw_in.at[l], dw_outt.at[l])

        for l in range(layers):
            h_in = xb.at[slot] if l == 0 else hid.at[l - 1]
            if l > 0:
                take_weights(l - 1, t, slot)

            def body(i, c, l=l, h_in=h_in):
                fwd(i, l, h_in)
                if l == 0:
                    @pl.when(jnp.logical_and(t >= 1, i == 0))
                    def _():
                        own_rows(1, t, slot, nxt)

                    @pl.when(jnp.logical_and(t >= 1, i == tiles - 1))
                    def _():
                        own_rows(0, t, slot, nxt)
                        start(bulk(1, nxt))
                return c

            lax.fori_loop(0, tiles, body, 0)
            if l == 0:
                @pl.when(jnp.logical_and(t >= 1, t < steps))
                def _():
                    start(bulk(0, slot))

                @pl.when(t == steps)
                def _():
                    for lb in reversed(range(layers - 1)):
                        last_trackers(lb, nxt)

        for l in reversed(range(layers)):
            h_in = xb.at[slot] if l == 0 else hid.at[l - 1]
            dw_in[l] = jnp.zeros_like(dw_in[l])
            dw_outt[l] = jnp.zeros_like(dw_outt[l])

            def body(i, c, l=l, h_in=h_in):
                bwd(i, l, h_in)
                return c

            lax.fori_loop(0, tiles, body, 0)
            if l > 0:
                gb_in[slot, l - 1] = dw_in[l].astype(BF16)
                gb_out[slot, l - 1] = dw_outt[l].T.astype(BF16)

                @pl.when(t < steps)
                def _():
                    for k in range(2):
                        gs[k][slot, l - 1, block(k, pos), :] = gb[k][slot, l - 1, block(k, pos), :]
                    start(g_swap(slot, l - 1))
            if l == 1:
                @pl.when(t == 0)
                def _():
                    for lb in reversed(range(layers - 1)):
                        wait(first_swap(lb))
                        for k in range(2):
                            sp[k][0, lb] = ps[k][lb].astype(BF16)
                        start(edges(0, 0, lb))

        @pl.when(t > 0)
        def _():
            wait(bulk(1, nxt))

        for k in range(2):
            g = (dw_in[0] if k == 0 else dw_outt[0].T).astype(BF16).astype(F32)

            @pl.when(t == 0)
            def _():
                y_st[k][0] = g

            @pl.when(t > 0)
            def _():
                y_st[k][0] = (mix0(y_st[k][0], 1, nxt, k) + g) - gold[k][...].astype(F32)

            gold[k][...] = g.astype(BF16)

        @pl.when(t < steps)
        def _():
            wait(bulk(0, slot))
            for k in range(2):
                y = y_st[k][0]
                yb[k][...] = y.astype(BF16)
                p = mix0(p_st[k][0], 0, slot, k) - LEARN_RATE * y
                p_st[k][0] = p
                pb[k][0] = p.astype(BF16)
        return carry

    lax.fori_loop(0, steps + 1, step, 0)
    new, old = steps % 2, (steps - 1) % 2
    for lb in reversed(range(layers - 1)):
        wait(y_swap_f32(lb))
        for k in range(2):
            y_st[k][lb + 1] = (y_st[k][lb + 1] + gb[k][new, lb].astype(F32)) - gb[k][old, lb].astype(F32)


def flush(*refs):
    copies = [pltpu.make_async_copy(refs[n], refs[4 + n], refs[8].at[n]) for n in range(4)]
    for cp in copies:
        cp.start()
    for cp in copies:
        cp.wait()


def solution(mesh):
    size_x = mesh.shape['tx']
    size_y = mesh.shape['ty']

    def device_fn(w_in, w_out, inputs, targets):
        _, _, layers, d, ff = w_in.shape
        steps = inputs.shape[2] - 1
        rows = inputs.shape[3]
        si, so = (d, ff), (ff, d)
        ei, eo = (d // LINE, ff), (ff // LINE, d)
        nb = layers - 1
        vm = pltpu.VMEM
        sem = pltpu.SemaphoreType.DMA
        any_spec = pl.BlockSpec(memory_space=pl.ANY)

        def both(lead, dtype):
            return [vm(lead + si, dtype), vm(lead + so, dtype)]

        outs = pl.pallas_call(
            functools.partial(kernel, (size_x, size_y, layers, steps)),
            out_shape=both((layers,), F32) * 2,
            in_specs=[any_spec] * 4,
            out_specs=[pl.BlockSpec(memory_space=pltpu.VMEM)] * 4,
            scratch_shapes=both((layers,), BF16) + both((), BF16) + both((2, 2, 3), BF16) + both((), BF16)
            + both((nb,), F32) * 2 + both((2, nb), BF16) * 4
            + [vm((2, 2, 2, nb) + ei, BF16), vm((2, 2, 2, nb) + eo, BF16)] + both((2, 2, nb), BF16)
            + [vm((layers,) + si, F32), vm((layers,) + si, F32),
               vm((2, rows, d), BF16), vm((2, rows, d), BF16), vm((layers - 1, rows, d), BF16),
               vm((layers, rows, d), BF16), vm((layers, rows, d), F32), vm((layers, rows, ff), F32),
               vm((layers, rows, ff), BF16), vm((rows, d), BF16),
               sem((2,)), sem((2, 2)), sem((2, 3, 2)), sem((2, 2, 3, 2)),
               sem((2, 3, 2 * nb)), sem((2, 2, 3, 2 * nb)),
               sem((2 * nb, 3)), sem((2 * nb, 3)), sem((2 * nb, 3)), sem((2 * nb, 3)), sem((2 * nb, 3)), sem((2 * nb, 3))],
            compiler_params=pltpu.CompilerParams(collective_id=0, has_side_effects=True, vmem_limit_bytes=56000000),
        )(w_in[0, 0], w_out[0, 0], inputs[0, 0], targets[0, 0])
        outs = pl.pallas_call(
            flush,
            out_shape=[jax.ShapeDtypeStruct(o.shape, o.dtype) for o in outs],
            in_specs=[pl.BlockSpec(memory_space=pltpu.VMEM)] * 4,
            out_specs=[any_spec] * 4,
            scratch_shapes=[sem((4,))],
        )(*[pltpu.with_memory_space_constraint(o, pltpu.VMEM) for o in outs])
        return tuple(o[None, None] for o in outs)

    block_spec = P('tx', 'ty')
    return jax.shard_map(device_fn, mesh=mesh, in_specs=(block_spec,) * 4, out_specs=(block_spec,) * 4, check_vma=False)
```

```python
import functools

import jax
import jax.numpy as jnp
from jax import lax
from jax.experimental import pallas as pl
from jax.experimental.pallas import tpu as pltpu
from jax.sharding import PartitionSpec as P

EPS = 1e-6
LEARN_RATE = 0.125
F32 = jnp.float32
BF16 = jnp.bfloat16
C0 = 0.7978845608028654
C1 = 0.7978845608028654 * 0.044715
TILE = 1024
LINE = 4
MESH = pl.DeviceIdType.MESH


def dot(a, b, dims):
    return lax.dot_general(a, b, (dims, ((), ())), preferred_element_type=F32)


def gelu_weight(z, z2):
    return 0.5 + 0.5 * jnp.tanh(z * (C0 + C1 * z2))


def forward_tile(rows, h_in, win, wout, u_ref, inv_ref, z_ref, w_ref, a_ref, before_out=None):
    d = h_in.shape[-1]
    hf = h_in[rows, :].astype(F32)
    ms = jnp.sum(hf * hf, axis=-1, keepdims=True) * (1.0 / d)
    inv = jnp.broadcast_to(lax.rsqrt(ms + EPS), hf.shape)
    inv_ref[rows, :] = inv
    u = (hf * inv).astype(BF16)
    u_ref[rows, :] = u
    z = dot(u, win[...], ((1,), (0,)))
    z_ref[rows, :] = z
    w = gelu_weight(z, z * z)
    w_ref[rows, :] = w
    a = (z * w).astype(BF16)
    a_ref[rows, :] = a
    if before_out is not None:
        before_out()
    mlp = dot(a, wout[...], ((1,), (0,)))
    return (hf + mlp).astype(BF16)


def backward_tile(rows, first, h_in, win, wout, u_ref, inv_ref, z_ref, w_ref, a_ref, dh_ref, dwin, dwoutt):
    d = dh_ref[rows, :]
    da = dot(d, wout[...], ((1,), (1,))).astype(BF16).astype(F32)
    z = z_ref[rows, :]
    z2 = z * z
    w = w_ref[rows, :]
    gp = w + (w - w * w) * (z * (2.0 * C0 + (6.0 * C1) * z2))
    dz = (da * gp).astype(BF16)
    a = a_ref[rows, :]
    dwoutt[...] += dot(d, a, ((0,), (0,)))
    dwin[...] += dot(u_ref[rows, :], dz, ((0,), (0,)))
    if not first:
        du = dot(dz, win[...], ((1,), (1,))).astype(BF16).astype(F32)
        hf = h_in[rows, :].astype(F32)
        inv = inv_ref[rows, :]
        s = jnp.sum(du * hf, axis=-1, keepdims=True) * (-1.0 / hf.shape[-1])
        dhf = d.astype(F32) + du * inv + hf * (inv * inv * inv * s)
        dh_ref[rows, :] = dhf.astype(BF16)


def kernel(dims, w_in, w_out, x_hbm, t_hbm, p_in, p_out, y_in, y_out,
           pb_in, pb_out, yb_in, yb_out, r_in, r_out, g_in, g_out,
           ps_in, ps_out, ys_in, ys_out, sp_in, sp_out, sy_in, sy_out,
           gb_in, gb_out, gs_in, gs_out, re_in, re_out, rp_in, rp_out,
           dw_in, dw_outt, xb, tb, hid, u_all, inv_all, z_all, w_all, a_all, dh,
           lsem, xsem, ssem, rsem, esend, erecv, gsend, grecv, psend, precv, fsend, frecv):
    size_x, size_y, layers, steps = dims
    rows_n = xb.shape[1]
    me_x = lax.axis_index('tx')
    me_y = lax.axis_index('ty')
    pos = lax.rem(me_x, LINE)
    line = me_x - pos

    def along(off):
        return {'tx': lax.rem(me_x + size_x + off, size_x), 'ty': me_y}

    other = {'tx': me_x, 'ty': lax.rem(me_y + 1, size_y)}
    near = (along(1), along(-1), other)
    ends = (along(LINE), along(-LINE), other)
    mates = [{'tx': line + lax.rem(pos + k, LINE), 'ty': me_y} for k in range(1, LINE)]
    p_st, y_st, pb, yb, rcv, gold = (p_in, p_out), (y_in, y_out), (pb_in, pb_out), (yb_in, yb_out), (r_in, r_out), (g_in, g_out)
    ps, ys, sp, sy = (ps_in, ps_out), (ys_in, ys_out), (sp_in, sp_out), (sy_in, sy_out)
    gb, gs, redge, rpart = (gb_in, gb_out), (gs_in, gs_out), (re_in, re_out), (rp_in, rp_out)
    blk = tuple(ref.shape[1] // LINE for ref in ps)

    def block(k, b):
        return pl.ds(pl.multiple_of(b * blk[k], blk[k]), blk[k])

    def remote(src, dst, s, r, dev):
        return pltpu.make_async_remote_copy(src_ref=src, dst_ref=dst, send_sem=s, recv_sem=r, device_id=dev, device_id_type=MESH)

    def start(copies):
        for cp in copies:
            cp.start()

    def wait(copies):
        for cp in copies:
            cp.wait()

    def loads():
        return [pltpu.make_async_copy(w_in, p_in, lsem.at[0]), pltpu.make_async_copy(w_out, p_out, lsem.at[1])]

    def batch(t, slot):
        return [pltpu.make_async_copy(x_hbm.at[t], xb.at[slot], xsem.at[slot, 0]),
                pltpu.make_async_copy(t_hbm.at[t], tb.at[slot], xsem.at[slot, 1])]

    def bulk(kind, par):
        return [remote((pb[k].at[0], yb[k])[kind], rcv[k].at[kind, par, d], ssem.at[kind, d, k], rsem.at[kind, par, d, k], near[d])
                for k in range(2) for d in range(3)]

    def mix0(v, kind, par, k):
        s = v + rcv[k][kind, par, 0].astype(F32)
        s = s + rcv[k][kind, par, 1].astype(F32)
        n = rcv[k][kind, par, 2].astype(F32)
        return (s + n + n) * 0.2

    def edges(kind, par, lb, ks=(0, 1)):
        out = []
        for k in ks:
            src = (sp, sy)[kind][k].at[par, lb]
            m = lb * 2 + k
            for d in range(3):
                part = (src.at[pl.ds((LINE - 1) * blk[k], blk[k])], src.at[pl.ds(0, blk[k])], src)[d]
                dst = redge[k].at[kind, par, d, lb] if d < 2 else rpart[k].at[kind, par, lb]
                out.append(remote(part, dst, esend.at[kind, d, m], erecv.at[kind, par, d, m], ends[d]))
        return out

    def swap(src, dst, send, recv, lb, ks=(0, 1)):
        out = []
        for k in ks:
            for n, dev in enumerate(mates):
                out.append(remote(src[k].at[block(k, lax.rem(pos + n + 1, LINE))], dst[k].at[block(k, pos)],
                                  send.at[lb * 2 + k, n], recv.at[lb * 2 + k, n], dev))
        return out

    def g_swap(par, lb, ks=(0, 1)):
        return swap([g.at[par, lb] for g in gb], [g.at[par, lb] for g in gs], gsend, grecv, lb, ks)

    def p_swap(par, lb, ks=(0, 1)):
        return swap([s.at[par, lb] for s in sp], [w.at[lb + 1] for w in pb], psend, precv, lb, ks)

    def p_swap_f32(lb, ks=(0, 1)):
        return swap([s.at[lb] for s in ps], [w.at[lb + 1] for w in p_st], psend, precv, lb, ks)

    def y_swap_f32(lb):
        return swap([s.at[lb] for s in ys], [w.at[lb + 1] for w in y_st], fsend, frecv, lb)

    def first_swap(lb):
        return swap([w.at[lb + 1] for w in (w_in, w_out)], [s.at[lb] for s in ps], fsend, frecv, lb)

    def mix_b(v, kind, par, lb, k, b):
        src = (sp, sy)[kind][k]
        rows = slice(b * blk[k], (b + 1) * blk[k])
        lo = redge[k][kind, par, 0, lb] if b == 0 else src[par, lb, (b - 1) * blk[k]:b * blk[k], :]
        hi = redge[k][kind, par, 1, lb] if b == LINE - 1 else src[par, lb, (b + 1) * blk[k]:(b + 2) * blk[k], :]
        n = rpart[k][kind, par, lb, rows, :].astype(F32)
        return (v + lo.astype(F32) + hi.astype(F32) + n + n) * 0.2

    def own_rows(lb, t, slot, nxt):
        wait(edges(0, nxt, lb))

        @pl.when(t >= 2)
        def _():
            wait(edges(1, slot, lb))

        for k in range(2):
            wait(g_swap(nxt, lb, (k,)))

            @pl.when(t == 1)
            def _():
                ys[k][lb] = gs[k][nxt, lb].astype(F32)

            @pl.when(t >= 2)
            def _():
                for b in range(LINE):
                    rows = slice(b * blk[k], (b + 1) * blk[k])
                    g = gs[k][nxt, lb, rows, :].astype(F32)
                    ys[k][lb, rows, :] = (mix_b(ys[k][lb, rows, :], 1, slot, lb, k, b) + g) - gs[k][slot, lb, rows, :].astype(F32)

            for b in range(LINE):
                rows = slice(b * blk[k], (b + 1) * blk[k])
                y = ys[k][lb, rows, :]
                p = mix_b(ps[k][lb, rows, :], 0, nxt, lb, k, b) - LEARN_RATE * y
                ps[k][lb, rows, :] = p
                sp[k][slot, lb, rows, :] = p.astype(BF16)
                sy[k][nxt, lb, rows, :] = y.astype(BF16)

            @pl.when(t < steps)
            def _():
                pb[k][lb + 1, block(k, pos), :] = sp[k][slot, lb, block(k, pos), :]
                start(p_swap(slot, lb, (k,)))

            @pl.when(t == steps)
            def _():
                p_st[k][lb + 1, block(k, pos), :] = ps[k][lb, block(k, pos), :]
                start(p_swap_f32(lb, (k,)))

        @pl.when(t < steps)
        def _():
            start(edges(0, slot, lb))

        start(edges(1, nxt, lb))

    def last_trackers(lb, par):
        wait(edges(1, par, lb))
        for k in range(2):
            for b in range(LINE):
                rows = slice(b * blk[k], (b + 1) * blk[k])
                ys[k][lb, rows, :] = mix_b(ys[k][lb, rows, :], 1, par, lb, k, b)
            y_st[k][lb + 1, block(k, pos), :] = ys[k][lb, block(k, pos), :]
        start(y_swap_f32(lb))

    def take_weights(lb, t, slot, ks):
        @pl.when(jnp.logical_and(t >= 1, t < steps))
        def _():
            wait(p_swap(slot, lb, ks))

        @pl.when(t == steps)
        def _():
            wait(p_swap_f32(lb, ks))
            for k in ks:
                pb[k][lb + 1] = p_st[k][lb + 1].astype(BF16)

    barrier = pltpu.get_barrier_semaphore()
    for peer in mates + list(near) + list(ends[:2]):
        pl.semaphore_signal(barrier, inc=1, device_id=peer, device_id_type=MESH)
    start(loads() + batch(0, 0))
    pl.semaphore_wait(barrier, LINE + 4)
    for lb in range(layers - 1):
        start(first_swap(lb))
    wait(loads())
    for k in range(2):
        for l in range(layers):
            pb[k][l] = p_st[k][l].astype(BF16)
        for lb in range(layers - 1):
            ps[k][lb, block(k, pos), :] = p_st[k][lb + 1, block(k, pos), :]
    start(bulk(0, 0))

    def step(t, carry):
        slot = lax.rem(t, 2)
        nxt = 1 - slot
        tiles = rows_n // TILE
        wait(batch(t, slot))

        @pl.when(t < steps)
        def _():
            start(batch(t + 1, nxt))

        def fwd(i, l, h_in, before_out=None):
            rows = pl.ds(i * TILE if isinstance(i, int) else pl.multiple_of(i * TILE, TILE), TILE)
            h = forward_tile(rows, h_in, pb_in.at[l], pb_out.at[l], u_all.at[l], inv_all.at[l], z_all.at[l], w_all.at[l], a_all.at[l], before_out)
            if l + 1 < layers:
                hid[l, rows, :] = h
            else:
                err = h.astype(F32) - tb[slot, rows, :].astype(F32)
                dh[rows, :] = (err * (2.0 / (rows_n * h.shape[-1]))).astype(BF16)

        def bwd(i, l, h_in):
            rows = pl.ds(pl.multiple_of(i * TILE, TILE), TILE)
            backward_tile(rows, l == 0, h_in, pb_in.at[l], pb_out.at[l], u_all.at[l], inv_all.at[l], z_all.at[l], w_all.at[l],
                          a_all.at[l], dh, dw_in.at[l], dw_outt.at[l])

        for l in range(layers):
            h_in = xb.at[slot] if l == 0 else hid.at[l - 1]
            if l > 0:
                take_weights(l - 1, t, slot, (0,) if l == 1 else (0, 1))

            def body(i, c, l=l, h_in=h_in):
                fwd(i, l, h_in)
                if l == 0:
                    @pl.when(jnp.logical_and(t >= 1, i == 0))
                    def _():
                        own_rows(1, t, slot, nxt)

                    @pl.when(jnp.logical_and(t >= 1, i == tiles - 1))
                    def _():
                        own_rows(0, t, slot, nxt)
                        start(bulk(1, nxt))
                return c

            if l == 1:
                fwd(0, l, h_in, lambda: take_weights(0, t, slot, (1,)))
            lax.fori_loop(1 if l == 1 else 0, tiles, body, 0)
            if l == 0:
                @pl.when(jnp.logical_and(t >= 1, t < steps))
                def _():
                    start(bulk(0, slot))

                @pl.when(t == steps)
                def _():
                    for lb in reversed(range(layers - 1)):
                        last_trackers(lb, nxt)

        for l in reversed(range(layers)):
            h_in = xb.at[slot] if l == 0 else hid.at[l - 1]
            dw_in[l] = jnp.zeros_like(dw_in[l])
            dw_outt[l] = jnp.zeros_like(dw_outt[l])

            def body(i, c, l=l, h_in=h_in):
                bwd(i, l, h_in)
                return c

            lax.fori_loop(0, tiles, body, 0)
            if l > 0:
                gb_in[slot, l - 1] = dw_in[l].astype(BF16)
                gb_out[slot, l - 1] = dw_outt[l].T.astype(BF16)

                @pl.when(t < steps)
                def _():
                    for k in range(2):
                        gs[k][slot, l - 1, block(k, pos), :] = gb[k][slot, l - 1, block(k, pos), :]
                    start(g_swap(slot, l - 1))
            if l == 1:
                @pl.when(t == 0)
                def _():
                    for lb in reversed(range(layers - 1)):
                        wait(first_swap(lb))
                        for k in range(2):
                            sp[k][0, lb] = ps[k][lb].astype(BF16)
                        start(edges(0, 0, lb))

        @pl.when(t > 0)
        def _():
            wait(bulk(1, nxt))

        for k in range(2):
            g = (dw_in[0] if k == 0 else dw_outt[0].T).astype(BF16).astype(F32)

            @pl.when(t == 0)
            def _():
                y_st[k][0] = g

            @pl.when(t > 0)
            def _():
                y_st[k][0] = (mix0(y_st[k][0], 1, nxt, k) + g) - gold[k][...].astype(F32)

            gold[k][...] = g.astype(BF16)

        @pl.when(t < steps)
        def _():
            wait(bulk(0, slot))
            for k in range(2):
                y = y_st[k][0]
                yb[k][...] = y.astype(BF16)
                p = mix0(p_st[k][0], 0, slot, k) - LEARN_RATE * y
                p_st[k][0] = p
                pb[k][0] = p.astype(BF16)
        return carry

    lax.fori_loop(0, steps + 1, step, 0)
    new, old = steps % 2, (steps - 1) % 2
    for lb in reversed(range(layers - 1)):
        wait(y_swap_f32(lb))
        for k in range(2):
            y_st[k][lb + 1] = (y_st[k][lb + 1] + gb[k][new, lb].astype(F32)) - gb[k][old, lb].astype(F32)


def flush(*refs):
    copies = [pltpu.make_async_copy(refs[n], refs[4 + n], refs[8].at[n]) for n in range(4)]
    for cp in copies:
        cp.start()
    for cp in copies:
        cp.wait()


def solution(mesh):
    size_x = mesh.shape['tx']
    size_y = mesh.shape['ty']

    def device_fn(w_in, w_out, inputs, targets):
        _, _, layers, d, ff = w_in.shape
        steps = inputs.shape[2] - 1
        rows = inputs.shape[3]
        si, so = (d, ff), (ff, d)
        ei, eo = (d // LINE, ff), (ff // LINE, d)
        nb = layers - 1
        vm = pltpu.VMEM
        sem = pltpu.SemaphoreType.DMA
        any_spec = pl.BlockSpec(memory_space=pl.ANY)

        def both(lead, dtype):
            return [vm(lead + si, dtype), vm(lead + so, dtype)]

        outs = pl.pallas_call(
            functools.partial(kernel, (size_x, size_y, layers, steps)),
            out_shape=both((layers,), F32) * 2,
            in_specs=[any_spec] * 4,
            out_specs=[pl.BlockSpec(memory_space=pltpu.VMEM)] * 4,
            scratch_shapes=both((layers,), BF16) + both((), BF16) + both((2, 2, 3), BF16) + both((), BF16)
            + both((nb,), F32) * 2 + both((2, nb), BF16) * 4
            + [vm((2, 2, 2, nb) + ei, BF16), vm((2, 2, 2, nb) + eo, BF16)] + both((2, 2, nb), BF16)
            + [vm((layers,) + si, F32), vm((layers,) + si, F32),
               vm((2, rows, d), BF16), vm((2, rows, d), BF16), vm((layers - 1, rows, d), BF16),
               vm((layers, rows, d), BF16), vm((layers, rows, d), F32), vm((layers, rows, ff), F32),
               vm((layers, rows, ff), F32), vm((layers, rows, ff), BF16), vm((rows, d), BF16),
               sem((2,)), sem((2, 2)), sem((2, 3, 2)), sem((2, 2, 3, 2)),
               sem((2, 3, 2 * nb)), sem((2, 2, 3, 2 * nb)),
               sem((2 * nb, 3)), sem((2 * nb, 3)), sem((2 * nb, 3)), sem((2 * nb, 3)), sem((2 * nb, 3)), sem((2 * nb, 3))],
            compiler_params=pltpu.CompilerParams(collective_id=0, has_side_effects=True, vmem_limit_bytes=62000000),
        )(w_in[0, 0], w_out[0, 0], inputs[0, 0], targets[0, 0])
        outs = pl.pallas_call(
            flush,
            out_shape=[jax.ShapeDtypeStruct(o.shape, o.dtype) for o in outs],
            in_specs=[pl.BlockSpec(memory_space=pltpu.VMEM)] * 4,
            out_specs=[any_spec] * 4,
            scratch_shapes=[sem((4,))],
        )(*[pltpu.with_memory_space_constraint(o, pltpu.VMEM) for o in outs])
        return tuple(o[None, None] for o in outs)

    block_spec = P('tx', 'ty')
    return jax.shard_map(device_fn, mesh=mesh, in_specs=(block_spec,) * 4, out_specs=(block_spec,) * 4, check_vma=False)
```

```python
import functools

import jax
import jax.numpy as jnp
from jax import lax
from jax.experimental import pallas as pl
from jax.experimental.pallas import tpu as pltpu
from jax.sharding import PartitionSpec as P

EPS = 1e-6
LEARN_RATE = 0.125
F32 = jnp.float32
BF16 = jnp.bfloat16
C0 = 0.7978845608028654
C1 = 0.7978845608028654 * 0.044715
TILE = 1024
LINE = 4
MESH = pl.DeviceIdType.MESH


def dot(a, b, dims):
    return lax.dot_general(a, b, (dims, ((), ())), preferred_element_type=F32)


def gelu_weight(z, z2):
    return 0.5 + 0.5 * jnp.tanh(z * (C0 + C1 * z2))


def normed(hf):
    ms = jnp.sum(hf * hf, axis=-1, keepdims=True) * (1.0 / hf.shape[-1])
    inv = jnp.broadcast_to(lax.rsqrt(ms + EPS), hf.shape)
    return inv, (hf * inv).astype(BF16)


def forward_tile(rows, h_in, win, wout, u_ref, inv_ref, z_ref, w_ref, a_ref, before_out=None):
    hf = h_in[rows, :].astype(F32)
    if inv_ref is None:
        u = u_ref[rows, :]
    else:
        inv_ref[rows, :], u = normed(hf)
        u_ref[rows, :] = u
    z = dot(u, win[...], ((1,), (0,)))
    z_ref[rows, :] = z
    w = gelu_weight(z, z * z)
    w_ref[rows, :] = w
    a = (z * w).astype(BF16)
    a_ref[rows, :] = a
    if before_out is not None:
        before_out()
    mlp = dot(a, wout[...], ((1,), (0,)))
    return (hf + mlp).astype(BF16)


def backward_tile(rows, first, h_in, win, wout, u_ref, inv_ref, z_ref, w_ref, a_ref, dh_ref, dwin, dwoutt):
    d = dh_ref[rows, :]
    da = dot(d, wout[...], ((1,), (1,))).astype(BF16).astype(F32)
    z = z_ref[rows, :]
    z2 = z * z
    w = w_ref[rows, :]
    gp = w + (w - w * w) * (z * (2.0 * C0 + (6.0 * C1) * z2))
    dz = (da * gp).astype(BF16)
    a = a_ref[rows, :]
    dwoutt[...] += dot(d, a, ((0,), (0,)))
    dwin[...] += dot(u_ref[rows, :], dz, ((0,), (0,)))
    if not first:
        du = dot(dz, win[...], ((1,), (1,))).astype(BF16).astype(F32)
        hf = h_in[rows, :].astype(F32)
        inv = inv_ref[rows, :]
        s = jnp.sum(du * hf, axis=-1, keepdims=True) * (-1.0 / hf.shape[-1])
        dhf = d.astype(F32) + du * inv + hf * (inv * inv * inv * s)
        dh_ref[rows, :] = dhf.astype(BF16)


def kernel(dims, w_in, w_out, x_hbm, t_hbm, p_in, p_out, y_in, y_out,
           pb_in, pb_out, yb_in, yb_out, r_in, r_out, g_in, g_out,
           ps_in, ps_out, ys_in, ys_out, sp_in, sp_out, sy_in, sy_out,
           gb_in, gb_out, gs_in, gs_out, re_in, re_out, rp_in, rp_out,
           dw_in, dw_outt, xb, tb, hid, u_first, u_all, inv_all, z_all, w_all, a_all, dh,
           lsem, xsem, ssem, rsem, esend, erecv, gsend, grecv, psend, precv, fsend, frecv):
    size_x, size_y, layers, steps = dims
    rows_n = xb.shape[1]
    me_x = lax.axis_index('tx')
    me_y = lax.axis_index('ty')
    pos = lax.rem(me_x, LINE)
    line = me_x - pos

    def along(off):
        return {'tx': lax.rem(me_x + size_x + off, size_x), 'ty': me_y}

    other = {'tx': me_x, 'ty': lax.rem(me_y + 1, size_y)}
    near = (along(1), along(-1), other)
    ends = (along(LINE), along(-LINE), other)
    mates = [{'tx': line + lax.rem(pos + k, LINE), 'ty': me_y} for k in range(1, LINE)]
    p_st, y_st, pb, yb, rcv, gold = (p_in, p_out), (y_in, y_out), (pb_in, pb_out), (yb_in, yb_out), (r_in, r_out), (g_in, g_out)
    ps, ys, sp, sy = (ps_in, ps_out), (ys_in, ys_out), (sp_in, sp_out), (sy_in, sy_out)
    gb, gs, redge, rpart = (gb_in, gb_out), (gs_in, gs_out), (re_in, re_out), (rp_in, rp_out)
    blk = tuple(ref.shape[1] // LINE for ref in ps)

    def block(k, b):
        return pl.ds(pl.multiple_of(b * blk[k], blk[k]), blk[k])

    def remote(src, dst, s, r, dev):
        return pltpu.make_async_remote_copy(src_ref=src, dst_ref=dst, send_sem=s, recv_sem=r, device_id=dev, device_id_type=MESH)

    def start(copies):
        for cp in copies:
            cp.start()

    def wait(copies):
        for cp in copies:
            cp.wait()

    def loads():
        return [pltpu.make_async_copy(w_in, p_in, lsem.at[0]), pltpu.make_async_copy(w_out, p_out, lsem.at[1])]

    def batch(t, slot):
        return [pltpu.make_async_copy(x_hbm.at[t], xb.at[slot], xsem.at[slot, 0]),
                pltpu.make_async_copy(t_hbm.at[t], tb.at[slot], xsem.at[slot, 1])]

    def bulk(kind, par):
        return [remote((pb[k].at[0], yb[k])[kind], rcv[k].at[kind, par, d], ssem.at[kind, d, k], rsem.at[kind, par, d, k], near[d])
                for k in range(2) for d in range(3)]

    def mix0(v, kind, par, k):
        s = v + rcv[k][kind, par, 0].astype(F32)
        s = s + rcv[k][kind, par, 1].astype(F32)
        n = rcv[k][kind, par, 2].astype(F32)
        return (s + n + n) * 0.2

    def edges(kind, par, lb, ks=(0, 1)):
        out = []
        for k in ks:
            src = (sp, sy)[kind][k].at[par, lb]
            m = lb * 2 + k
            for d in range(3):
                part = (src.at[pl.ds((LINE - 1) * blk[k], blk[k])], src.at[pl.ds(0, blk[k])], src)[d]
                dst = redge[k].at[kind, par, d, lb] if d < 2 else rpart[k].at[kind, par, lb]
                out.append(remote(part, dst, esend.at[kind, d, m], erecv.at[kind, par, d, m], ends[d]))
        return out

    def swap(src, dst, send, recv, lb, ks=(0, 1)):
        out = []
        for k in ks:
            for n, dev in enumerate(mates):
                out.append(remote(src[k].at[block(k, lax.rem(pos + n + 1, LINE))], dst[k].at[block(k, pos)],
                                  send.at[lb * 2 + k, n], recv.at[lb * 2 + k, n], dev))
        return out

    def g_swap(par, lb, ks=(0, 1)):
        return swap([g.at[par, lb] for g in gb], [g.at[par, lb] for g in gs], gsend, grecv, lb, ks)

    def p_swap(par, lb, ks=(0, 1)):
        return swap([s.at[par, lb] for s in sp], [w.at[lb + 1] for w in pb], psend, precv, lb, ks)

    def p_swap_f32(lb, ks=(0, 1)):
        return swap([s.at[lb] for s in ps], [w.at[lb + 1] for w in p_st], psend, precv, lb, ks)

    def y_swap_f32(lb):
        return swap([s.at[lb] for s in ys], [w.at[lb + 1] for w in y_st], fsend, frecv, lb)

    def first_swap(lb):
        return swap([w.at[lb + 1] for w in (w_in, w_out)], [s.at[lb] for s in ps], fsend, frecv, lb)

    def mix_b(v, kind, par, lb, k, b):
        src = (sp, sy)[kind][k]
        rows = slice(b * blk[k], (b + 1) * blk[k])
        lo = redge[k][kind, par, 0, lb] if b == 0 else src[par, lb, (b - 1) * blk[k]:b * blk[k], :]
        hi = redge[k][kind, par, 1, lb] if b == LINE - 1 else src[par, lb, (b + 1) * blk[k]:(b + 2) * blk[k], :]
        n = rpart[k][kind, par, lb, rows, :].astype(F32)
        return (v + lo.astype(F32) + hi.astype(F32) + n + n) * 0.2

    def own_rows(lb, t, slot, nxt):
        wait(edges(0, nxt, lb))

        @pl.when(t >= 2)
        def _():
            wait(edges(1, slot, lb))

        for k in range(2):
            wait(g_swap(nxt, lb, (k,)))

            @pl.when(t == 1)
            def _():
                ys[k][lb] = gs[k][nxt, lb].astype(F32)

            @pl.when(t >= 2)
            def _():
                for b in range(LINE):
                    rows = slice(b * blk[k], (b + 1) * blk[k])
                    g = gs[k][nxt, lb, rows, :].astype(F32)
                    ys[k][lb, rows, :] = (mix_b(ys[k][lb, rows, :], 1, slot, lb, k, b) + g) - gs[k][slot, lb, rows, :].astype(F32)

            for b in range(LINE):
                rows = slice(b * blk[k], (b + 1) * blk[k])
                y = ys[k][lb, rows, :]
                p = mix_b(ps[k][lb, rows, :], 0, nxt, lb, k, b) - LEARN_RATE * y
                ps[k][lb, rows, :] = p
                sp[k][slot, lb, rows, :] = p.astype(BF16)
                sy[k][nxt, lb, rows, :] = y.astype(BF16)

            @pl.when(t < steps)
            def _():
                pb[k][lb + 1, block(k, pos), :] = sp[k][slot, lb, block(k, pos), :]
                start(p_swap(slot, lb, (k,)))

            @pl.when(t == steps)
            def _():
                p_st[k][lb + 1, block(k, pos), :] = ps[k][lb, block(k, pos), :]
                start(p_swap_f32(lb, (k,)))

        @pl.when(t < steps)
        def _():
            start(edges(0, slot, lb))

        start(edges(1, nxt, lb))

    def last_trackers(lb, par):
        wait(edges(1, par, lb))
        for k in range(2):
            for b in range(LINE):
                rows = slice(b * blk[k], (b + 1) * blk[k])
                ys[k][lb, rows, :] = mix_b(ys[k][lb, rows, :], 1, par, lb, k, b)
            y_st[k][lb + 1, block(k, pos), :] = ys[k][lb, block(k, pos), :]
        start(y_swap_f32(lb))

    def take_weights(lb, t, slot, ks):
        @pl.when(jnp.logical_and(t >= 1, t < steps))
        def _():
            wait(p_swap(slot, lb, ks))

        @pl.when(t == steps)
        def _():
            wait(p_swap_f32(lb, ks))
            for k in ks:
                pb[k][lb + 1] = p_st[k][lb + 1].astype(BF16)

    barrier = pltpu.get_barrier_semaphore()
    for peer in mates + list(near) + list(ends[:2]):
        pl.semaphore_signal(barrier, inc=1, device_id=peer, device_id_type=MESH)
    start(loads() + batch(0, 0))
    pl.semaphore_wait(barrier, LINE + 4)
    for lb in range(layers - 1):
        start(first_swap(lb))
    wait(loads())
    for k in range(2):
        for l in range(layers):
            pb[k][l] = p_st[k][l].astype(BF16)
        for lb in range(layers - 1):
            ps[k][lb, block(k, pos), :] = p_st[k][lb + 1, block(k, pos), :]
    start(bulk(0, 0))

    tiles = rows_n // TILE

    def prepare(t, slot):
        wait(batch(t, slot))

        def body(i, c):
            rows = pl.ds(pl.multiple_of(i * TILE, TILE), TILE)
            u_first[slot, rows, :] = normed(xb[slot, rows, :].astype(F32))[1]
            return c

        lax.fori_loop(0, tiles, body, 0)

    prepare(0, 0)

    def step(t, carry):
        slot = lax.rem(t, 2)
        nxt = 1 - slot
        @pl.when(t < steps)
        def _():
            start(batch(t + 1, nxt))

        def acts(l):
            return (u_first.at[slot], None) if l == 0 else (u_all.at[l - 1], inv_all.at[l - 1])

        def fwd(i, l, h_in, before_out=None):
            rows = pl.ds(i * TILE if isinstance(i, int) else pl.multiple_of(i * TILE, TILE), TILE)
            h = forward_tile(rows, h_in, pb_in.at[l], pb_out.at[l], *acts(l), z_all.at[l], w_all.at[l], a_all.at[l], before_out)
            if l + 1 < layers:
                hid[l, rows, :] = h
            else:
                err = h.astype(F32) - tb[slot, rows, :].astype(F32)
                dh[rows, :] = (err * (2.0 / (rows_n * h.shape[-1]))).astype(BF16)

        def bwd(i, l, h_in):
            rows = pl.ds(pl.multiple_of(i * TILE, TILE), TILE)
            backward_tile(rows, l == 0, h_in, pb_in.at[l], pb_out.at[l], *acts(l), z_all.at[l], w_all.at[l],
                          a_all.at[l], dh, dw_in.at[l], dw_outt.at[l])

        for l in range(layers):
            h_in = xb.at[slot] if l == 0 else hid.at[l - 1]
            if l == 1:
                dw_in[...] = jnp.zeros_like(dw_in)
                dw_outt[...] = jnp.zeros_like(dw_outt)

                @pl.when(t < steps)
                def _():
                    prepare(t + 1, nxt)

            if l > 0:
                take_weights(l - 1, t, slot, (0,) if l == 1 else (0, 1))

            def body(i, c, l=l, h_in=h_in):
                fwd(i, l, h_in)
                if l == 0:
                    @pl.when(jnp.logical_and(t >= 1, i == 0))
                    def _():
                        own_rows(1, t, slot, nxt)

                    @pl.when(jnp.logical_and(t >= 1, i == tiles - 1))
                    def _():
                        own_rows(0, t, slot, nxt)
                        start(bulk(1, nxt))
                return c

            if l == 1:
                fwd(0, l, h_in, lambda: take_weights(0, t, slot, (1,)))
            lax.fori_loop(1 if l == 1 else 0, tiles, body, 0)
            if l == 0:
                @pl.when(jnp.logical_and(t >= 1, t < steps))
                def _():
                    start(bulk(0, slot))

                @pl.when(t == steps)
                def _():
                    for lb in reversed(range(layers - 1)):
                        last_trackers(lb, nxt)

        for l in reversed(range(layers)):
            h_in = xb.at[slot] if l == 0 else hid.at[l - 1]
            def body(i, c, l=l, h_in=h_in):
                bwd(i, l, h_in)
                return c

            lax.fori_loop(0, tiles, body, 0)
            if l > 0:
                gb_in[slot, l - 1] = dw_in[l].astype(BF16)
                gb_out[slot, l - 1] = dw_outt[l].T.astype(BF16)

                @pl.when(t < steps)
                def _():
                    for k in range(2):
                        gs[k][slot, l - 1, block(k, pos), :] = gb[k][slot, l - 1, block(k, pos), :]
                    start(g_swap(slot, l - 1))
            if l == 1:
                @pl.when(t == 0)
                def _():
                    for lb in reversed(range(layers - 1)):
                        wait(first_swap(lb))
                        for k in range(2):
                            sp[k][0, lb] = ps[k][lb].astype(BF16)
                        start(edges(0, 0, lb))

        @pl.when(t > 0)
        def _():
            wait(bulk(1, nxt))

        for k in range(2):
            g = (dw_in[0] if k == 0 else dw_outt[0].T).astype(BF16).astype(F32)

            @pl.when(t == 0)
            def _():
                y_st[k][0] = g

            @pl.when(t > 0)
            def _():
                y_st[k][0] = (mix0(y_st[k][0], 1, nxt, k) + g) - gold[k][...].astype(F32)

            gold[k][...] = g.astype(BF16)

        @pl.when(t < steps)
        def _():
            wait(bulk(0, slot))
            for k in range(2):
                y = y_st[k][0]
                yb[k][...] = y.astype(BF16)
                p = mix0(p_st[k][0], 0, slot, k) - LEARN_RATE * y
                p_st[k][0] = p
                pb[k][0] = p.astype(BF16)
        return carry

    lax.fori_loop(0, steps + 1, step, 0)
    new, old = steps % 2, (steps - 1) % 2
    for lb in reversed(range(layers - 1)):
        wait(y_swap_f32(lb))
        for k in range(2):
            y_st[k][lb + 1] = (y_st[k][lb + 1] + gb[k][new, lb].astype(F32)) - gb[k][old, lb].astype(F32)


def flush(*refs):
    copies = [pltpu.make_async_copy(refs[n], refs[4 + n], refs[8].at[n]) for n in range(4)]
    for cp in copies:
        cp.start()
    for cp in copies:
        cp.wait()


def solution(mesh):
    size_x = mesh.shape['tx']
    size_y = mesh.shape['ty']

    def device_fn(w_in, w_out, inputs, targets):
        _, _, layers, d, ff = w_in.shape
        steps = inputs.shape[2] - 1
        rows = inputs.shape[3]
        si, so = (d, ff), (ff, d)
        ei, eo = (d // LINE, ff), (ff // LINE, d)
        nb = layers - 1
        vm = pltpu.VMEM
        sem = pltpu.SemaphoreType.DMA
        any_spec = pl.BlockSpec(memory_space=pl.ANY)

        def both(lead, dtype):
            return [vm(lead + si, dtype), vm(lead + so, dtype)]

        outs = pl.pallas_call(
            functools.partial(kernel, (size_x, size_y, layers, steps)),
            out_shape=both((layers,), F32) * 2,
            in_specs=[any_spec] * 4,
            out_specs=[pl.BlockSpec(memory_space=pltpu.VMEM)] * 4,
            scratch_shapes=both((layers,), BF16) + both((), BF16) + both((2, 2, 3), BF16) + both((), BF16)
            + both((nb,), F32) * 2 + both((2, nb), BF16) * 4
            + [vm((2, 2, 2, nb) + ei, BF16), vm((2, 2, 2, nb) + eo, BF16)] + both((2, 2, nb), BF16)
            + [vm((layers,) + si, F32), vm((layers,) + si, F32),
               vm((2, rows, d), BF16), vm((2, rows, d), BF16), vm((layers - 1, rows, d), BF16),
               vm((2, rows, d), BF16), vm((layers - 1, rows, d), BF16), vm((layers - 1, rows, d), F32), vm((layers, rows, ff), F32),
               vm((layers, rows, ff), F32), vm((layers, rows, ff), BF16), vm((rows, d), BF16),
               sem((2,)), sem((2, 2)), sem((2, 3, 2)), sem((2, 2, 3, 2)),
               sem((2, 3, 2 * nb)), sem((2, 2, 3, 2 * nb)),
               sem((2 * nb, 3)), sem((2 * nb, 3)), sem((2 * nb, 3)), sem((2 * nb, 3)), sem((2 * nb, 3)), sem((2 * nb, 3))],
            compiler_params=pltpu.CompilerParams(collective_id=0, has_side_effects=True, vmem_limit_bytes=62000000),
        )(w_in[0, 0], w_out[0, 0], inputs[0, 0], targets[0, 0])
        outs = pl.pallas_call(
            flush,
            out_shape=[jax.ShapeDtypeStruct(o.shape, o.dtype) for o in outs],
            in_specs=[pl.BlockSpec(memory_space=pltpu.VMEM)] * 4,
            out_specs=[any_spec] * 4,
            scratch_shapes=[sem((4,))],
        )(*[pltpu.with_memory_space_constraint(o, pltpu.VMEM) for o in outs])
        return tuple(o[None, None] for o in outs)

    block_spec = P('tx', 'ty')
    return jax.shard_map(device_fn, mesh=mesh, in_specs=(block_spec,) * 4, out_specs=(block_spec,) * 4, check_vma=False)
```

```python
import functools

import jax
import jax.numpy as jnp
from jax import lax
from jax.experimental import pallas as pl
from jax.experimental.pallas import tpu as pltpu
from jax.sharding import PartitionSpec as P

EPS = 1e-6
LEARN_RATE = 0.125
F32 = jnp.float32
BF16 = jnp.bfloat16
C0 = 0.7978845608028654
C1 = 0.7978845608028654 * 0.044715
TILE = 1024
LINE = 4
MESH = pl.DeviceIdType.MESH


def dot(a, b, dims):
    return lax.dot_general(a, b, (dims, ((), ())), preferred_element_type=F32)


def gelu_weight(z, z2):
    return 0.5 + 0.5 * jnp.tanh(z * (C0 + C1 * z2))


def normed(hf):
    ms = jnp.sum(hf * hf, axis=-1, keepdims=True) * (1.0 / hf.shape[-1])
    inv = jnp.broadcast_to(lax.rsqrt(ms + EPS), hf.shape)
    return inv, (hf * inv).astype(BF16)


def forward_tile(rows, h_in, win, wout, u_ref, inv_ref, z_ref, w_ref, a_ref, before_out=None):
    hf = h_in[rows, :].astype(F32)
    if inv_ref is None:
        u = u_ref[rows, :]
    else:
        inv_ref[rows, :], u = normed(hf)
        u_ref[rows, :] = u
    z = dot(u, win[...], ((1,), (0,)))
    z_ref[rows, :] = z
    w = gelu_weight(z, z * z)
    w_ref[rows, :] = w
    a = (z * w).astype(BF16)
    a_ref[rows, :] = a
    if before_out is not None:
        before_out()
    mlp = dot(a, wout[...], ((1,), (0,)))
    return (hf + mlp).astype(BF16)


def backward_tile(rows, first, h_in, win, wout, u_ref, inv_ref, z_ref, w_ref, a_ref, dh_ref, dwin, dwoutt):
    d = dh_ref[rows, :]
    da = dot(d, wout[...], ((1,), (1,))).astype(BF16).astype(F32)
    z = z_ref[rows, :]
    z2 = z * z
    w = w_ref[rows, :]
    gp = w + (w - w * w) * (z * (2.0 * C0 + (6.0 * C1) * z2))
    dz = (da * gp).astype(BF16)
    a = a_ref[rows, :]
    dwoutt[...] += dot(d, a, ((0,), (0,)))
    dwin[...] += dot(u_ref[rows, :], dz, ((0,), (0,)))
    if not first:
        du = dot(dz, win[...], ((1,), (1,))).astype(BF16).astype(F32)
        hf = h_in[rows, :].astype(F32)
        inv = inv_ref[rows, :]
        s = jnp.sum(du * hf, axis=-1, keepdims=True) * (-1.0 / hf.shape[-1])
        dhf = d.astype(F32) + du * inv + hf * (inv * inv * inv * s)
        dh_ref[rows, :] = dhf.astype(BF16)


def kernel(dims, w_in, w_out, x_hbm, t_hbm, p_in, p_out, y_in, y_out,
           pb_in, pb_out, yb_in, yb_out, r_in, r_out, g_in, g_out,
           ps_in, ps_out, ys_in, ys_out, sp_in, sp_out, sy_in, sy_out,
           gb_in, gb_out, gs_in, gs_out, re_in, re_out, rp_in, rp_out,
           dw_in, dw_outt, xb, tb, hid, u_first, u_all, inv_all, z_all, w_all, a_all, dh,
           lsem, xsem, ssem, rsem, esend, erecv, gsend, grecv, psend, precv, fsend, frecv):
    size_x, size_y, layers, steps = dims
    rows_n = xb.shape[1]
    me_x = lax.axis_index('tx')
    me_y = lax.axis_index('ty')
    pos = lax.rem(me_x, LINE)
    line = me_x - pos

    def along(off):
        return {'tx': lax.rem(me_x + size_x + off, size_x), 'ty': me_y}

    other = {'tx': me_x, 'ty': lax.rem(me_y + 1, size_y)}
    near = (along(1), along(-1), other)
    ends = (along(LINE), along(-LINE), other)
    mates = [{'tx': line + lax.rem(pos + k, LINE), 'ty': me_y} for k in range(1, LINE)]
    p_st, y_st, pb, yb, rcv, gold = (p_in, p_out), (y_in, y_out), (pb_in, pb_out), (yb_in, yb_out), (r_in, r_out), (g_in, g_out)
    ps, ys, sp, sy = (ps_in, ps_out), (ys_in, ys_out), (sp_in, sp_out), (sy_in, sy_out)
    gb, gs, redge, rpart = (gb_in, gb_out), (gs_in, gs_out), (re_in, re_out), (rp_in, rp_out)
    blk = tuple(ref.shape[1] // LINE for ref in ps)

    def block(k, b):
        return pl.ds(pl.multiple_of(b * blk[k], blk[k]), blk[k])

    def remote(src, dst, s, r, dev):
        return pltpu.make_async_remote_copy(src_ref=src, dst_ref=dst, send_sem=s, recv_sem=r, device_id=dev, device_id_type=MESH)

    def start(copies):
        for cp in copies:
            cp.start()

    def wait(copies):
        for cp in copies:
            cp.wait()

    def loads():
        return [pltpu.make_async_copy(w_in, p_in, lsem.at[0]), pltpu.make_async_copy(w_out, p_out, lsem.at[1])]

    def batch(t, slot):
        return [pltpu.make_async_copy(x_hbm.at[t], xb.at[slot], xsem.at[slot, 0]),
                pltpu.make_async_copy(t_hbm.at[t], tb.at[slot], xsem.at[slot, 1])]

    def bulk(kind, par):
        return [remote((pb[k].at[0], yb[k])[kind], rcv[k].at[kind, par, d], ssem.at[kind, d, k], rsem.at[kind, par, d, k], near[d])
                for k in range(2) for d in range(3)]

    def mix0(v, kind, par, k):
        s = v + rcv[k][kind, par, 0].astype(F32)
        s = s + rcv[k][kind, par, 1].astype(F32)
        n = rcv[k][kind, par, 2].astype(F32)
        return (s + n + n) * 0.2

    def edges(kind, par, lb, ks=(0, 1)):
        out = []
        for k in ks:
            src = (sp, sy)[kind][k].at[par, lb]
            m = lb * 2 + k
            for d in range(3):
                part = (src.at[pl.ds((LINE - 1) * blk[k], blk[k])], src.at[pl.ds(0, blk[k])], src)[d]
                dst = redge[k].at[kind, par, d, lb] if d < 2 else rpart[k].at[kind, par, lb]
                out.append(remote(part, dst, esend.at[kind, d, m], erecv.at[kind, par, d, m], ends[d]))
        return out

    def swap(src, dst, send, recv, lb, ks=(0, 1)):
        out = []
        for k in ks:
            for n, dev in enumerate(mates):
                out.append(remote(src[k].at[block(k, lax.rem(pos + n + 1, LINE))], dst[k].at[block(k, pos)],
                                  send.at[lb * 2 + k, n], recv.at[lb * 2 + k, n], dev))
        return out

    def g_swap(par, lb, ks=(0, 1)):
        return swap([g.at[par, lb] for g in gb], [g.at[par, lb] for g in gs], gsend, grecv, lb, ks)

    def p_swap(par, lb, ks=(0, 1)):
        return swap([s.at[par, lb] for s in sp], [w.at[lb + 1] for w in pb], psend, precv, lb, ks)

    def p_swap_f32(lb, ks=(0, 1)):
        return swap([s.at[lb] for s in ps], [w.at[lb + 1] for w in p_st], psend, precv, lb, ks)

    def y_swap_f32(lb):
        return swap([s.at[lb] for s in ys], [w.at[lb + 1] for w in y_st], fsend, frecv, lb)

    def first_swap(lb):
        return swap([w.at[lb + 1] for w in (w_in, w_out)], [s.at[lb] for s in ps], fsend, frecv, lb)

    def mix_b(v, kind, par, lb, k, b):
        src = (sp, sy)[kind][k]
        rows = slice(b * blk[k], (b + 1) * blk[k])
        lo = redge[k][kind, par, 0, lb] if b == 0 else src[par, lb, (b - 1) * blk[k]:b * blk[k], :]
        hi = redge[k][kind, par, 1, lb] if b == LINE - 1 else src[par, lb, (b + 1) * blk[k]:(b + 2) * blk[k], :]
        n = rpart[k][kind, par, lb, rows, :].astype(F32)
        return (v + lo.astype(F32) + hi.astype(F32) + n + n) * 0.2

    def own_rows(lb, t, slot, nxt):
        wait(edges(0, nxt, lb))

        @pl.when(t >= 2)
        def _():
            wait(edges(1, slot, lb))

        for k in range(2):
            wait(g_swap(nxt, lb, (k,)))

            @pl.when(t == 1)
            def _():
                ys[k][lb] = gs[k][nxt, lb].astype(F32)

            @pl.when(t >= 2)
            def _():
                for b in range(LINE):
                    rows = slice(b * blk[k], (b + 1) * blk[k])
                    g = gs[k][nxt, lb, rows, :].astype(F32)
                    ys[k][lb, rows, :] = (mix_b(ys[k][lb, rows, :], 1, slot, lb, k, b) + g) - gs[k][slot, lb, rows, :].astype(F32)

            for b in range(LINE):
                rows = slice(b * blk[k], (b + 1) * blk[k])
                y = ys[k][lb, rows, :]
                p = mix_b(ps[k][lb, rows, :], 0, nxt, lb, k, b) - LEARN_RATE * y
                ps[k][lb, rows, :] = p
                sp[k][slot, lb, rows, :] = p.astype(BF16)

            @pl.when(t < steps)
            def _():
                pb[k][lb + 1, block(k, pos), :] = sp[k][slot, lb, block(k, pos), :]
                start(p_swap(slot, lb, (k,)))

            @pl.when(t == steps)
            def _():
                p_st[k][lb + 1, block(k, pos), :] = ps[k][lb, block(k, pos), :]
                start(p_swap_f32(lb, (k,)))

            sy[k][nxt, lb] = ys[k][lb].astype(BF16)

        @pl.when(t < steps)
        def _():
            start(edges(0, slot, lb))

        start(edges(1, nxt, lb))

    def last_trackers(lb, par):
        wait(edges(1, par, lb))
        for k in range(2):
            for b in range(LINE):
                rows = slice(b * blk[k], (b + 1) * blk[k])
                ys[k][lb, rows, :] = mix_b(ys[k][lb, rows, :], 1, par, lb, k, b)
            y_st[k][lb + 1, block(k, pos), :] = ys[k][lb, block(k, pos), :]
        start(y_swap_f32(lb))

    def take_weights(lb, t, slot, ks):
        @pl.when(jnp.logical_and(t >= 1, t < steps))
        def _():
            wait(p_swap(slot, lb, ks))

        @pl.when(t == steps)
        def _():
            wait(p_swap_f32(lb, ks))
            for k in ks:
                pb[k][lb + 1] = p_st[k][lb + 1].astype(BF16)

    barrier = pltpu.get_barrier_semaphore()
    for peer in mates + list(near) + list(ends[:2]):
        pl.semaphore_signal(barrier, inc=1, device_id=peer, device_id_type=MESH)
    start(loads() + batch(0, 0))
    pl.semaphore_wait(barrier, LINE + 4)
    for lb in range(layers - 1):
        start(first_swap(lb))
    wait(loads())
    for k in range(2):
        for l in range(layers):
            pb[k][l] = p_st[k][l].astype(BF16)
        for lb in range(layers - 1):
            ps[k][lb, block(k, pos), :] = p_st[k][lb + 1, block(k, pos), :]
    start(bulk(0, 0))

    tiles = rows_n // TILE

    def prepare(t, slot):
        wait(batch(t, slot))

        def body(i, c):
            rows = pl.ds(pl.multiple_of(i * TILE, TILE), TILE)
            u_first[slot, rows, :] = normed(xb[slot, rows, :].astype(F32))[1]
            return c

        lax.fori_loop(0, tiles, body, 0)

    prepare(0, 0)

    def step(t, carry):
        slot = lax.rem(t, 2)
        nxt = 1 - slot
        @pl.when(t < steps)
        def _():
            start(batch(t + 1, nxt))

        def acts(l):
            return (u_first.at[slot], None) if l == 0 else (u_all.at[l - 1], inv_all.at[l - 1])

        def fwd(i, l, h_in, before_out=None):
            rows = pl.ds(i * TILE if isinstance(i, int) else pl.multiple_of(i * TILE, TILE), TILE)
            h = forward_tile(rows, h_in, pb_in.at[l], pb_out.at[l], *acts(l), z_all.at[l], w_all.at[l], a_all.at[l], before_out)
            if l + 1 < layers:
                hid[l, rows, :] = h
            else:
                err = h.astype(F32) - tb[slot, rows, :].astype(F32)
                dh[rows, :] = (err * (2.0 / (rows_n * h.shape[-1]))).astype(BF16)

        def bwd(i, l, h_in):
            rows = pl.ds(pl.multiple_of(i * TILE, TILE), TILE)
            backward_tile(rows, l == 0, h_in, pb_in.at[l], pb_out.at[l], *acts(l), z_all.at[l], w_all.at[l],
                          a_all.at[l], dh, dw_in.at[l], dw_outt.at[l])

        for l in range(layers):
            h_in = xb.at[slot] if l == 0 else hid.at[l - 1]
            if l == 1:
                dw_in[...] = jnp.zeros_like(dw_in)
                dw_outt[...] = jnp.zeros_like(dw_outt)

                @pl.when(t < steps)
                def _():
                    prepare(t + 1, nxt)

            if l > 0:
                take_weights(l - 1, t, slot, (0,) if l == 1 else (0, 1))

            def body(i, c, l=l, h_in=h_in):
                fwd(i, l, h_in)
                if l == 0:
                    @pl.when(jnp.logical_and(t >= 1, i == 0))
                    def _():
                        own_rows(1, t, slot, nxt)

                    @pl.when(jnp.logical_and(t >= 1, i == tiles - 1))
                    def _():
                        own_rows(0, t, slot, nxt)
                        start(bulk(1, nxt))
                return c

            if l == 1:
                fwd(0, l, h_in, lambda: take_weights(0, t, slot, (1,)))
            lax.fori_loop(1 if l == 1 else 0, tiles, body, 0)
            if l == 0:
                @pl.when(jnp.logical_and(t >= 1, t < steps))
                def _():
                    start(bulk(0, slot))

                @pl.when(t == steps)
                def _():
                    for lb in reversed(range(layers - 1)):
                        last_trackers(lb, nxt)

        for l in reversed(range(layers)):
            h_in = xb.at[slot] if l == 0 else hid.at[l - 1]
            def body(i, c, l=l, h_in=h_in):
                bwd(i, l, h_in)
                return c

            lax.fori_loop(0, tiles, body, 0)
            if l > 0:
                gb_in[slot, l - 1] = dw_in[l].astype(BF16)
                gb_out[slot, l - 1] = dw_outt[l].T.astype(BF16)

                @pl.when(t < steps)
                def _():
                    for k in range(2):
                        gs[k][slot, l - 1, block(k, pos), :] = gb[k][slot, l - 1, block(k, pos), :]
                    start(g_swap(slot, l - 1))
            if l == 1:
                @pl.when(t == 0)
                def _():
                    for lb in reversed(range(layers - 1)):
                        wait(first_swap(lb))
                        for k in range(2):
                            sp[k][0, lb] = ps[k][lb].astype(BF16)
                        start(edges(0, 0, lb))

        @pl.when(t > 0)
        def _():
            wait(bulk(1, nxt))

        for k in range(2):
            g = (dw_in[0] if k == 0 else dw_outt[0].T).astype(BF16).astype(F32)

            @pl.when(t == 0)
            def _():
                y_st[k][0] = g

            @pl.when(t > 0)
            def _():
                y_st[k][0] = (mix0(y_st[k][0], 1, nxt, k) + g) - gold[k][...].astype(F32)

            gold[k][...] = g.astype(BF16)

        @pl.when(t < steps)
        def _():
            wait(bulk(0, slot))
            for k in range(2):
                y = y_st[k][0]
                yb[k][...] = y.astype(BF16)
                p = mix0(p_st[k][0], 0, slot, k) - LEARN_RATE * y
                p_st[k][0] = p
                pb[k][0] = p.astype(BF16)
        return carry

    lax.fori_loop(0, steps + 1, step, 0)
    new, old = steps % 2, (steps - 1) % 2
    for lb in reversed(range(layers - 1)):
        wait(y_swap_f32(lb))
        for k in range(2):
            y_st[k][lb + 1] = (y_st[k][lb + 1] + gb[k][new, lb].astype(F32)) - gb[k][old, lb].astype(F32)


def flush(*refs):
    copies = [pltpu.make_async_copy(refs[n], refs[4 + n], refs[8].at[n]) for n in range(4)]
    for cp in copies:
        cp.start()
    for cp in copies:
        cp.wait()


def solution(mesh):
    size_x = mesh.shape['tx']
    size_y = mesh.shape['ty']

    def device_fn(w_in, w_out, inputs, targets):
        _, _, layers, d, ff = w_in.shape
        steps = inputs.shape[2] - 1
        rows = inputs.shape[3]
        si, so = (d, ff), (ff, d)
        ei, eo = (d // LINE, ff), (ff // LINE, d)
        nb = layers - 1
        vm = pltpu.VMEM
        sem = pltpu.SemaphoreType.DMA
        any_spec = pl.BlockSpec(memory_space=pl.ANY)

        def both(lead, dtype):
            return [vm(lead + si, dtype), vm(lead + so, dtype)]

        outs = pl.pallas_call(
            functools.partial(kernel, (size_x, size_y, layers, steps)),
            out_shape=both((layers,), F32) * 2,
            in_specs=[any_spec] * 4,
            out_specs=[pl.BlockSpec(memory_space=pltpu.VMEM)] * 4,
            scratch_shapes=both((layers,), BF16) + both((), BF16) + both((2, 2, 3), BF16) + both((), BF16)
            + both((nb,), F32) * 2 + both((2, nb), BF16) * 4
            + [vm((2, 2, 2, nb) + ei, BF16), vm((2, 2, 2, nb) + eo, BF16)] + both((2, 2, nb), BF16)
            + [vm((layers,) + si, F32), vm((layers,) + si, F32),
               vm((2, rows, d), BF16), vm((2, rows, d), BF16), vm((layers - 1, rows, d), BF16),
               vm((2, rows, d), BF16), vm((layers - 1, rows, d), BF16), vm((layers - 1, rows, d), F32), vm((layers, rows, ff), F32),
               vm((layers, rows, ff), F32), vm((layers, rows, ff), BF16), vm((rows, d), BF16),
               sem((2,)), sem((2, 2)), sem((2, 3, 2)), sem((2, 2, 3, 2)),
               sem((2, 3, 2 * nb)), sem((2, 2, 3, 2 * nb)),
               sem((2 * nb, 3)), sem((2 * nb, 3)), sem((2 * nb, 3)), sem((2 * nb, 3)), sem((2 * nb, 3)), sem((2 * nb, 3))],
            compiler_params=pltpu.CompilerParams(collective_id=0, has_side_effects=True, vmem_limit_bytes=62000000),
        )(w_in[0, 0], w_out[0, 0], inputs[0, 0], targets[0, 0])
        outs = pl.pallas_call(
            flush,
            out_shape=[jax.ShapeDtypeStruct(o.shape, o.dtype) for o in outs],
            in_specs=[pl.BlockSpec(memory_space=pltpu.VMEM)] * 4,
            out_specs=[any_spec] * 4,
            scratch_shapes=[sem((4,))],
        )(*[pltpu.with_memory_space_constraint(o, pltpu.VMEM) for o in outs])
        return tuple(o[None, None] for o in outs)

    block_spec = P('tx', 'ty')
    return jax.shard_map(device_fn, mesh=mesh, in_specs=(block_spec,) * 4, out_specs=(block_spec,) * 4, check_vma=False)
```
